256 devices in a mesh: groups: 2 (over z), expert: 64 (over y, x), tensor: 2 (over core).
Axes of the slice: x: 8, y: 8, z: 2, core: 2. Of those that a mesh axis runs over, the one named last changes fastest.
The devices are a block of a 8x8x16 slice.
Arguments:
- tokens: bfloat16 [1024, 6144], P(('groups', 'expert')), parts along dimension 0, may hold values from -6 to 6
- routes: int32 [1024, 2], P(('groups', 'expert')), parts along dimension 0, may hold values from 0 to 3, all different within a row; in each aligned block of 8 rows (0 to 7, 8 to 15, ...) at most 5 rows name the same one
- router_logits: float32 [1024, 4], P(('groups', 'expert')), parts along dimension 0, may hold values from -9 to 310
- gate_weight: bfloat16 [64, 6144, 512], P('expert', None, 'tensor'), may hold values from -0.078125 to 0.078125
- up_weight: bfloat16 [64, 6144, 512], P('expert', None, 'tensor'), may hold values from -0.078125 to 0.078125
- down_weight: bfloat16 [64, 512, 6144], P('expert', 'tensor'), may hold values from -0.0625 to 0.0625
Outputs:
- layer_out: bfloat16 [1024, 6144], P(('groups', 'expert'), 'tensor'), parts along dimension 0
The draws below stay inside these ranges and needn't reach their ends.
There are 2 independent parts, one for each index of `groups`. The reference program is written for one: setup_inputs(seed, part) draws one part's arguments, and reference() takes and returns one part's arrays. A program takes and returns all parts, laid end to end along the dimension named above; an argument that names none is the same for every part. Nothing has to cross between parts.
Inputs may be any that keep to these rules, and one draw needn't show every extreme that they name: `routes`: each row names two different experts. In the rows of one index of expert (aligned blocks of 8 rows) no expert is named more than 5 times, and in every draw some block names some expert exactly 5 times.
All inputs are finite; a program needn't handle non-finite values.
Results may differ from the reference program's by a relative error of at most 0.0049.
Values may be sent and summed in bfloat16 or wider, within the bound.
A program may use at most 64 MiB of HBM per device.

```python
import math
from functools import partial
import jax
import jax.numpy as jnp
import numpy as np
from jax import lax

D = 6144
EXPERTS = 4
TOK_DEV = 8
SEGS = 16
FF = 8192
CAP = 5
TOKENS = 512
N_EXPERT = 64


def draw_router_logits(key, part):
    first_key, second_key, third_key = jax.random.split(key, 3)
    base = jnp.clip(jax.random.normal(first_key, (TOKENS, EXPERTS), jnp.float32) * 1.5, -9.0, 9.0)
    return base


def level_of(own_key, extent, cuts, smallest, high):
    factor_of, own = 1.0, jax.random.fold_in(own_key, 6)
    for axis_at, parts in cuts:
        steps = jnp.exp(jax.random.uniform(jax.random.fold_in(own, axis_at), (parts,), jnp.float32, smallest / len(cuts), high / len(cuts)))
        factor_of = factor_of * jnp.repeat(steps, extent[axis_at] // parts).reshape([-1 if axis == axis_at else 1 for axis in range(len(extent))])
    return factor_of


def deal_out(stream_key, own, number, rows, number_of, top, reach, slope):
    ranking = jax.random.permutation(stream_key, number_of)
    packed, usual = load_shares(number_of, rows * top, reach, slope, True), load_shares(number_of, rows * top, reach, slope, False)
    places = jnp.arange(number_of)

    def named(lengths, rotation):
        used = int((lengths > 0).sum())
        fixed = max(1, used // 4)
        passed = fixed + (places - fixed + rotation * (used - fixed)) % max(1, number_of - fixed)
        return jnp.zeros((number_of,), jnp.int32).at[ranking[jnp.where(places < fixed, places, passed)]].set(jnp.asarray(lengths, jnp.int32))

    lengths = jnp.where(number % 4 == 0, named(packed, number // 4), named(usual, number - number // 4 - 1))
    mixed = jax.random.permutation(jax.random.fold_in(own, 3), number_of)
    giver, receiver = mixed[0:number_of // 2 * 2:2], mixed[1:number_of // 2 * 2:2]
    margin = jnp.minimum(lengths[giver] - 1, reach - lengths[receiver]) // 2
    margin = jnp.where((giver == ranking[0]) | (receiver == ranking[0]) | (lengths[receiver] == 0), 0, jnp.maximum(margin, 0))
    passed = jax.random.randint(jax.random.fold_in(own, 4), (number_of // 2,), 0, 1 << 20) % (margin + 1)
    lengths = lengths.at[giver].add(-passed).at[receiver].add(passed)
    items = jnp.searchsorted(jnp.cumsum(lengths), jnp.arange(rows * top), side="right").astype(jnp.int32)
    table = items.reshape(top, rows).T
    table = table[jax.random.permutation(jax.random.fold_in(own, 1), rows)]
    rotation = jax.random.randint(jax.random.fold_in(own, 2), (rows, 1), 0, top)
    return jnp.take_along_axis(table, (jnp.arange(top)[None, :] + rotation) % top, axis=1)


def load_shares(amount, total, limit, skew, full):
    loads = [(1 << 20) // math.isqrt(grade ** skew) + 1 for grade in range(1, amount + 1)]
    largest = limit if full else min(limit, max(-(-total // amount), total * loads[0] // sum(loads)))
    least = 1 if total - largest >= amount - 1 else 0
    holding, surplus = [largest] + [least] * (amount - 1), total - largest - least * (amount - 1)
    while surplus > 0:
        movable = [i for i in range(1, amount) if holding[i] < largest] or [i for i in range(1, amount) if holding[i] < limit]
        whole, left = sum([loads[i] for i in movable]), surplus
        for i in movable:
            more = min(limit - holding[i], max(1, left * loads[i] // whole), surplus)
            holding[i] = holding[i] + more
            surplus = surplus - more
    return np.array(holding)


def gaussian(own_key, extent, scale, reach, pieces=(), kind=jnp.bfloat16):
    factor_of = level_of(own_key, extent, pieces, -0.22, 0.18) if pieces else 1.0
    entries = jax.random.normal(own_key, extent, jnp.float32) * scale * factor_of
    return jnp.minimum(jnp.maximum(entries, -reach), reach).astype(kind)


def setup_inputs(seed: int = 0, part: int = 0) -> dict:
    streams_of = jax.random.split(jax.random.key(seed), 7)
    part_keys = jax.random.split(jax.random.fold_in(streams_of[6], part), 7)
    tokens = gaussian(part_keys[0], (TOKENS, D), 1.0, 6.0, ((0, 64),))
    routes_keys = jax.random.split(jax.random.fold_in(part_keys[1], 1), TOKENS // TOK_DEV)
    routes_turns = jax.random.permutation(jax.random.fold_in(part_keys[1], 3), TOKENS // TOK_DEV)
    routes = jax.vmap(lambda own, number: deal_out(jax.random.fold_in(part_keys[1], 2), own, number, TOK_DEV, EXPERTS, 2, CAP, 2))(routes_keys, routes_turns).reshape((TOKENS, 2))
    router_logits = draw_router_logits(jax.random.fold_in(jax.random.fold_in(streams_of[6], part), 71), part)
    gate_weight = gaussian(streams_of[3], (N_EXPERT, D, FF // SEGS), D ** -0.5, 0.078125, ((0, 64), (2, 2)))
    up_weight = gaussian(streams_of[4], (N_EXPERT, D, FF // SEGS), D ** -0.5, 0.078125, ((0, 64), (2, 2)))
    down_weight = gaussian(streams_of[5], (N_EXPERT, FF // SEGS, D), FF ** -0.5, 0.0625, ((0, 64), (1, 2)))
    return dict(tokens=tokens, routes=routes, router_logits=router_logits, gate_weight=gate_weight, up_weight=up_weight, down_weight=down_weight)


def expert_block(expert, tokens, source_token, gate_weight, up_weight, down_weight):
    first = expert * SEGS
    gate_part = lax.dynamic_slice_in_dim(gate_weight, first, SEGS, 0)
    up_part = lax.dynamic_slice_in_dim(up_weight, first, SEGS, 0)
    down_part = lax.dynamic_slice_in_dim(down_weight, first, SEGS, 0)
    block_width = gate_part.shape[2]
    gate_full = jnp.transpose(gate_part, (1, 0, 2)).reshape(D, SEGS * block_width)
    up_full = jnp.transpose(up_part, (1, 0, 2)).reshape(D, SEGS * block_width)
    down_full = down_part.reshape(SEGS * block_width, D)
    row_ids = lax.dynamic_index_in_dim(source_token, expert, 0, keepdims=False)
    inputs = jnp.take(tokens, row_ids, axis=0)
    gate_out = jnp.dot(inputs, gate_full, preferred_element_type=jnp.float32)
    up_out = jnp.dot(inputs, up_full, preferred_element_type=jnp.float32)
    hidden = (jax.nn.silu(gate_out) * up_out).astype(jnp.bfloat16)
    return jnp.dot(hidden, down_full, preferred_element_type=jnp.float32)


def reference(tokens, routes, router_logits, gate_weight, up_weight, down_weight):
    token_count = tokens.shape[0]
    block_count = token_count // TOK_DEV
    picked = jnp.take_along_axis(router_logits, routes, axis=1)
    route_weight = jax.nn.softmax(picked, axis=1)
    expert_ids = jnp.arange(EXPERTS, dtype=jnp.int32)
    onehot = (routes[:, :, None] == expert_ids[None, None, :]).astype(jnp.int32)
    per_block = onehot.reshape(block_count, TOK_DEV * 2, EXPERTS)
    earlier = (jnp.cumsum(per_block, axis=1) - per_block).astype(jnp.int32)
    slot_index = jnp.sum(earlier * per_block, axis=2).astype(jnp.int32).reshape(token_count, 2)
    block_of = (jnp.arange(token_count, dtype=jnp.int32) // TOK_DEV)[:, None]
    slots_each = block_count * CAP
    slot_global = (routes * slots_each + block_of * CAP + slot_index).astype(jnp.int32)
    token_ids = jnp.repeat(jnp.arange(token_count, dtype=jnp.int32), 2)
    source_token = jnp.zeros((EXPERTS * slots_each,), jnp.int32).at[slot_global.reshape(-1)].set(token_ids)
    source_token = source_token.reshape(EXPERTS, slots_each)
    compute = partial(expert_block, tokens=tokens, source_token=source_token, gate_weight=gate_weight, up_weight=up_weight, down_weight=down_weight)
    expert_out = lax.map(compute, expert_ids)
    expert_out = expert_out.reshape(EXPERTS * slots_each, D)
    picked_rows = jnp.take(expert_out, slot_global.reshape(-1), axis=0).reshape(token_count, 2, D)
    layer_out = jnp.sum(route_weight[:, :, None] * picked_rows, axis=1)
    return layer_out.astype(jnp.bfloat16)
```

```python
import functools
import math

import jax
import jax.numpy as jnp
from jax import lax
from jax.experimental import pallas as pl
from jax.experimental.pallas import tpu as pltpu
from jax.sharding import PartitionSpec as P

MESH = pl.DeviceIdType.MESH
F32, BF16 = jnp.float32, jnp.bfloat16
LANES = 128


def ring_order(side):
    order = [0]
    for k in range(1, side // 2):
        order += [k, side - k]
    return order + [side // 2]


def kernel(
    side, segs, tok, wrow, gate, up, down, out,
    gu, wd, own, sib, pre, hid, hmir, hsib, wall, wcol, part, csend, crecv, fsend, frecv,
    load_sem, p1_send, p1_recv, ring_send, ring_recv, d2d_send, d2d_recv,
    w1_send, w1_recv, w2_send, w2_recv, x_send, x_recv,
    cr_send, cr_recv, f_send, f_recv,
):
    order = ring_order(side)
    pos = {k: p for p, k in enumerate(order)}
    mirror = [pos[(side - k) % side] for k in order]
    cuts = [0, 1] + list(range(3, side - 2, 2)) + [side]
    blocks = list(zip(cuts[:-1], cuts[1:]))
    nb = len(blocks)
    rows, width = own.shape[3], own.shape[4]
    hc = wd.shape[1]
    hops = (side // 2, side // 2 - 1)

    core = lax.axis_index("tensor")
    place = lax.axis_index("expert")
    y, x = place // side, lax.rem(place, side)
    expert = place // segs
    sign = 1 - 2 * core

    def along(axis, k):
        step = sign * k + side
        if axis == 0:
            return {"expert": lax.rem(y + step, side) * side + x}
        return {"expert": y * side + lax.rem(x + step, side)}

    def remote(src, dst, send, recv, device):
        return pltpu.make_async_remote_copy(
            src_ref=src, dst_ref=dst, send_sem=send, recv_sem=recv, device_id=device, device_id_type=MESH
        )

    other = {"tensor": 1 - core}
    started = []

    def start(copy):
        copy.start()
        started.append(copy)

    def arrived(ref, send, recv):
        remote(ref, ref, send, recv, other).wait_recv()

    half = 2 * width
    tok_loads = [
        pltpu.make_async_copy(
            tok.at[:, pl.ds(pl.multiple_of(core * half + t * width, LANES), width)], own.at[t, 0, 0], load_sem.at[t]
        )
        for t in range(2)
    ]
    w_load = pltpu.make_async_copy(wrow, wall.at[0, 0], load_sem.at[2])
    for copy in tok_loads:
        copy.start()
    w_load.start()
    loads = []
    for q in range(4):
        who = core if q < 2 else 1 - core
        first = pl.multiple_of(who * half + (q % 2) * width, LANES)
        for i, matrix in enumerate((gate, up)):
            loads.append(
                pltpu.make_async_copy(
                    matrix.at[0, pl.ds(first, width), :], gu.at[q, :, pl.ds(i * hc, hc)], load_sem.at[4 + 2 * q + i]
                )
            )
    for copy in loads:
        copy.start()
    wd_load = pltpu.make_async_copy(
        down.at[0, :, pl.ds(pl.multiple_of(core * half, LANES), half)], wd.at[0], load_sem.at[3]
    )
    wd_load.start()

    barrier = pltpu.get_barrier_semaphore()
    for k in range(1, side):
        for axis in range(2):
            pl.semaphore_signal(barrier, inc=1, device_id=along(axis, k), device_id_type=MESH)
    pl.semaphore_signal(barrier, inc=1, device_id=other, device_id_type=MESH)
    pre[...] = jnp.zeros_like(pre)
    for copy in tok_loads:
        copy.wait()
    w_load.wait()
    pl.semaphore_wait(barrier, 2 * (side - 1) + 1)

    for k in order[1:]:
        back = pos[side - k]
        for t in range(2):
            start(remote(own.at[t, 0, 0], own.at[t, 0, back], p1_send.at[t, back], p1_recv.at[t, back], along(t, k)))
    def forward(t, d, h, b):
        lo, hi = blocks[b]
        k = (side - h) % side if d == 0 else h
        k_there = (side - h - 1) % side if d == 0 else h + 1
        start(remote(
            own.at[t, pos[k], lo:hi], own.at[t, pos[k_there], lo:hi],
            ring_send.at[t, d, h, b], ring_recv.at[t, pos[k_there], b], along(1 - t, 1 if d == 0 else side - 1),
        ))

    def project(src, t, q, chunk, mirrored):
        r = jnp.dot(src[t, chunk].reshape(side * rows, width), gu[q], preferred_element_type=F32)
        r = r.reshape(side, rows, 2 * hc)
        for p in range(side):
            at = (mirror[chunk], mirror[p]) if mirrored else (chunk, p)
            i, j = at if t == 0 else at[::-1]
            pre[i, j] += r[p]

    def own_dot(t, chunk):
        project(own, t, t, chunk, False)

    def sib_dot(t, chunk):
        arrived(sib.at[t, chunk], d2d_send.at[t, chunk], d2d_recv.at[t, chunk])
        project(sib, t, 2 + t, chunk, True)

    waiting = []
    loaded = False
    for step in range(side // 2 + nb):
        complete = []
        for h in reversed(range(side // 2 + 1)):
            b = step - h
            if b < 0 or b >= nb:
                continue
            lo, hi = blocks[b]
            for t in range(2):
                if h == 0:
                    for p in range(max(lo, 1), hi):
                        arrived(own.at[t, 0, p], p1_send.at[t, p], p1_recv.at[t, p])
                    for d in range(2):
                        forward(t, d, 0, b)
                    if b == nb - 1:
                        complete.append((t, 0))
                    continue
                for d in range(2):
                    if h > hops[d]:
                        continue
                    chunk = pos[(side - h) % side if d == 0 else h]
                    arrived(own.at[t, chunk, lo:hi], ring_send.at[t, 0, 0, b], ring_recv.at[t, chunk, b])
                    if h < hops[d]:
                        forward(t, d, h, b)
                    if b == nb - 1:
                        complete.append((t, chunk))
        for t, chunk in complete:
            start(remote(own.at[t, chunk], sib.at[t, chunk], d2d_send.at[t, chunk], d2d_recv.at[t, chunk], other))
        if step == 0:
            start(remote(
                down.at[0, :, pl.ds(pl.multiple_of((1 - core) * half, LANES), half)], wd.at[1],
                x_send.at[0], x_recv.at[0], other,
            ))
            for k in order[1:]:
                back = pos[side - k]
                start(remote(wall.at[0, 0], wall.at[0, back], w1_send.at[back], w1_recv.at[back], along(0, k)))
        if step == nb - 1:
            for p in range(1, side):
                arrived(wall.at[0, p], w1_send.at[p], w1_recv.at[p])
            for k in order[1:]:
                back = pos[side - k]
                start(remote(wall.at[0], wall.at[back], w2_send.at[back], w2_recv.at[back], along(1, k)))
        if (complete or waiting) and not loaded:
            for copy in loads:
                copy.wait()
            loaded = True
        for t, chunk in complete:
            own_dot(t, chunk)
        for t, chunk in waiting:
            sib_dot(t, chunk)
        waiting = complete
    for t, chunk in waiting:
        sib_dot(t, chunk)

    for i in range(side):
        g, u = pre[i, :, :, :hc], pre[i, :, :, hc:]
        h_here = (g / (1.0 + jnp.exp(-g)) * u).astype(BF16)
        hid[i] = h_here
        for j in range(side):
            hmir[mirror[i], mirror[j]] = h_here[j]
    start(remote(hmir, hsib, x_send.at[1], x_recv.at[1], other))

    for p in range(1, side):
        arrived(wall.at[p], w2_send.at[p], w2_recv.at[p])
    lane = lax.broadcasted_iota(jnp.int32, (side, rows, LANES), 2)
    row = lax.broadcasted_iota(jnp.int32, (side, rows, LANES), 1)
    for i in range(side):
        spread = jnp.broadcast_to(wall[i], (side, rows, LANES))
        wcol[i] = jnp.sum(jnp.where(lane == expert * rows + row, spread, 0.0), axis=2, keepdims=True)

    wd_load.wait()
    arrived(wd.at[1], x_send.at[0], x_recv.at[0])
    arrived(hsib, x_send.at[1], x_recv.at[1])

    def make_part(t, chunk):
        if t == 0:
            a, b, scale = hid[chunk], hsib[chunk], wcol[chunk]
        else:
            a, b, scale = hid[:, chunk], hsib[:, chunk], wcol[:, chunk]
        cols = slice(t * width, (t + 1) * width)
        r = jnp.dot(a.reshape(side * rows, hc), wd[0, :, cols], preferred_element_type=F32)
        r += jnp.dot(b.reshape(side * rows, hc), wd[1, :, cols], preferred_element_type=F32)
        part[t, chunk] = r.reshape(side, rows, width) * scale

    back_blocks = blocks[::-1]
    made = set()

    def need(t, k):
        if (t, k) not in made:
            made.add((t, k))
            make_part(t, pos[k])

    for step in range(side // 2 + nb):
        for h in reversed(range(side // 2 + 1)):
            b = step - h
            if b < 0 or b >= nb:
                continue
            lo, hi = back_blocks[b]
            for t in range(2):
                if h == side // 2:
                    need(t, 0)
                    arrived(crecv.at[t, 0, h, lo:hi], cr_send.at[t, 0, 0, b], cr_recv.at[t, 0, h, b])
                    arrived(crecv.at[t, 1, h - 1, lo:hi], cr_send.at[t, 0, 0, b], cr_recv.at[t, 1, h - 1, b])
                    total = (
                        part[t, 0, lo:hi]
                        + crecv[t, 0, h, lo:hi].astype(F32)
                        + crecv[t, 1, h - 1, lo:hi].astype(F32)
                    )
                    part[t, 0, lo:hi] = total
                    fsend[t, lo:hi] = total.astype(BF16)
                    for p in reversed(range(max(lo, 1), hi)):
                        k = order[p]
                        back = pos[side - k]
                        start(remote(fsend.at[t, p], frecv.at[t, back], f_send.at[t, back], f_recv.at[t, back], along(t, k)))
                    continue
                for d in range(2):
                    if h >= hops[d]:
                        continue
                    k = hops[d] - h if d == 0 else side - hops[d] + h
                    need(t, k)
                    value = part[t, pos[k], lo:hi]
                    if h > 0:
                        arrived(crecv.at[t, d, h, lo:hi], cr_send.at[t, 0, 0, b], cr_recv.at[t, d, h, b])
                        value = value + crecv[t, d, h, lo:hi].astype(F32)
                    csend[t, d, h, lo:hi] = value.astype(BF16)
                    start(remote(
                        csend.at[t, d, h, lo:hi], crecv.at[t, d, h + 1, lo:hi],
                        cr_send.at[t, d, h, b], cr_recv.at[t, d, h + 1, b], along(1 - t, 1 if d == 0 else side - 1),
                    ))
    for t in range(2):
        total = part[t, 0, 0]
        for p in range(1, side):
            arrived(frecv.at[t, p], f_send.at[t, p], f_recv.at[t, p])
            total = total + frecv[t, p].astype(F32)
        out[:, t * width:(t + 1) * width] = total.astype(out.dtype)
    for copy in started:
        copy.wait_send()


def solution(mesh):
    n_expert = mesh.shape["expert"]
    side = math.isqrt(n_expert)
    nb = len([0, 1] + list(range(3, side - 2, 2)))

    def layer(tokens, routes, router_logits, gate_weight, up_weight, down_weight):
        rows, width = tokens.shape[0], tokens.shape[1] // 4
        experts = router_logits.shape[1]
        hc = down_weight.shape[1]
        named = routes[:, :, None] == jnp.arange(experts, dtype=jnp.int32)
        picked = jnp.sum(jnp.where(named, router_logits[:, None, :], 0.0), axis=2)
        weight = jnp.sum(jnp.where(named, jax.nn.softmax(picked, axis=1)[:, :, None], 0.0), axis=1)
        wrow = jnp.pad(weight.T.reshape(1, experts * rows), ((0, 0), (0, LANES - experts * rows)))
        hop = side // 2
        dma = pltpu.SemaphoreType.DMA
        scratch = [
            pltpu.VMEM((4, width, 2 * hc), BF16),
            pltpu.VMEM((2, hc, 2 * width), BF16),
            pltpu.VMEM((2, side, side, rows, width), BF16),
            pltpu.VMEM((2, side, side, rows, width), BF16),
            pltpu.VMEM((side, side, rows, 2 * hc), F32),
            pltpu.VMEM((side, side, rows, hc), BF16),
            pltpu.VMEM((side, side, rows, hc), BF16),
            pltpu.VMEM((side, side, rows, hc), BF16),
            pltpu.VMEM((side, side, 1, LANES), F32),
            pltpu.VMEM((side, side, rows, 1), F32),
            pltpu.VMEM((2, side, side, rows, width), F32),
            pltpu.VMEM((2, 2, hop, side, rows, width), BF16),
            pltpu.VMEM((2, 2, hop + 1, side, rows, width), BF16),
            pltpu.VMEM((2, side, rows, width), BF16),
            pltpu.VMEM((2, side, rows, width), BF16),
            dma((12,)),
            dma((2, side)), dma((2, side)),
            dma((2, 2, hop, nb)), dma((2, side, nb)),
            dma((2, side)), dma((2, side)),
            dma((side,)), dma((side,)), dma((side,)), dma((side,)),
            dma((2,)), dma((2,)),
            dma((2, 2, hop, nb)), dma((2, 2, hop + 1, nb)),
            dma((2, side)), dma((2, side)),
        ]
        hbm = pl.BlockSpec(memory_space=pl.ANY)
        return pl.pallas_call(
            functools.partial(kernel, side, n_expert // experts),
            out_shape=jax.ShapeDtypeStruct((rows, 2 * width), BF16),
            in_specs=[hbm] * 5,
            out_specs=pl.BlockSpec(memory_space=pltpu.VMEM),
            scratch_shapes=scratch,
            compiler_params=pltpu.CompilerParams(
                collective_id=0, has_side_effects=True, vmem_limit_bytes=60 * 1024 * 1024
            ),
            name="moe_layer",
        )(tokens, wrow, gate_weight, up_weight, down_weight)

    return jax.shard_map(
        layer,
        mesh=mesh,
        in_specs=(
            P(("groups", "expert"), None),
            P(("groups", "expert"), None),
            P(("groups", "expert"), None),
            P("expert", None, "tensor"),
            P("expert", None, "tensor"),
            P("expert", "tensor", None),
        ),
        out_specs=P(("groups", "expert"), "tensor"),
        check_vma=False,
    )
```

```python
import functools
import math

import jax
import jax.numpy as jnp
from jax import lax
from jax.experimental import pallas as pl
from jax.experimental.pallas import tpu as pltpu
from jax.sharding import PartitionSpec as P

MESH = pl.DeviceIdType.MESH
F32, BF16 = jnp.float32, jnp.bfloat16
LANES = 128


def ring_order(side):
    order = [0]
    for k in range(1, side // 2):
        order += [k, side - k]
    return order + [side // 2]


def kernel(
    side, segs, tok, routes, logits, gate, up, down, out,
    named, scores, gu, wd, own, sib, pre, hid, hmir, hsib, wall, wcol, part, csend, crecv, fsend, frecv,
    load_sem, p1_send, p1_recv, ring_send, ring_recv, d2d_send, d2d_recv,
    w1_send, w1_recv, w2_send, w2_recv, x_send, x_recv,
    cr_send, cr_recv, f_send, f_recv,
):
    order = ring_order(side)
    pos = {k: p for p, k in enumerate(order)}
    mirror = [pos[(side - k) % side] for k in order]
    cuts = [0] + list(range(1, side, 2)) + [side]
    blocks = list(zip(cuts[:-1], cuts[1:]))
    nb = len(blocks)
    rows, width = own.shape[3], own.shape[4]
    hc = wd.shape[1]
    hops = (side // 2, side // 2 - 1)

    core = lax.axis_index("tensor")
    place = lax.axis_index("expert")
    y, x = place // side, lax.rem(place, side)
    expert = place // segs
    sign = 1 - 2 * core

    def along(axis, k):
        step = sign * k + side
        if axis == 0:
            return {"expert": lax.rem(y + step, side) * side + x}
        return {"expert": y * side + lax.rem(x + step, side)}

    def remote(src, dst, send, recv, device):
        return pltpu.make_async_remote_copy(
            src_ref=src, dst_ref=dst, send_sem=send, recv_sem=recv, device_id=device, device_id_type=MESH
        )

    other = {"tensor": 1 - core}
    started = []

    def start(copy):
        copy.start()
        started.append(copy)

    def arrived(ref, send, recv):
        remote(ref, ref, send, recv, other).wait_recv()

    half = 2 * width
    tok_loads = [
        pltpu.make_async_copy(
            tok.at[:, pl.ds(pl.multiple_of(core * half + t * width, LANES), width)], own.at[t, 0, 0], load_sem.at[t]
        )
        for t in range(2)
    ]
    small_loads = [
        pltpu.make_async_copy(routes, named, load_sem.at[2]),
        pltpu.make_async_copy(logits, scores, load_sem.at[12]),
    ]
    for copy in tok_loads + small_loads:
        copy.start()
    loads = []
    for q in range(4):
        who = core if q < 2 else 1 - core
        first = pl.multiple_of(who * half + (q % 2) * width, LANES)
        for i, matrix in enumerate((gate, up)):
            loads.append(
                pltpu.make_async_copy(
                    matrix.at[0, pl.ds(first, width), :], gu.at[q, :, pl.ds(i * hc, hc)], load_sem.at[4 + 2 * q + i]
                )
            )
    for copy in loads:
        copy.start()
    wd_load = pltpu.make_async_copy(
        down.at[0, :, pl.ds(pl.multiple_of(core * half, LANES), half)], wd.at[0], load_sem.at[3]
    )
    wd_load.start()

    barrier = pltpu.get_barrier_semaphore()
    for k in (1, side - 1):
        for axis in range(2):
            pl.semaphore_signal(barrier, inc=1, device_id=along(axis, k), device_id_type=MESH)
    pl.semaphore_signal(barrier, inc=1, device_id=other, device_id_type=MESH)
    for copy in tok_loads:
        copy.wait()
    pl.semaphore_wait(barrier, 5)

    def pass_on(t, d, h):
        k = (side - h) % side if d == 0 else h
        k_there = side - h - 1 if d == 0 else h + 1
        start(remote(
            own.at[t, 0, pos[k]], own.at[t, 0, pos[k_there]],
            p1_send.at[t, pos[k_there]], p1_recv.at[t, pos[k_there]], along(t, 1 if d == 0 else side - 1),
        ))

    def forward(t, d, h, b):
        lo, hi = blocks[b]
        k = (side - h) % side if d == 0 else h
        k_there = (side - h - 1) % side if d == 0 else h + 1
        start(remote(
            own.at[t, pos[k], lo:hi], own.at[t, pos[k_there], lo:hi],
            ring_send.at[t, d, h, b], ring_recv.at[t, pos[k_there], b], along(1 - t, 1 if d == 0 else side - 1),
        ))

    def project(src, t, q, chunk, mirrored):
        r = jnp.dot(src[t, chunk].reshape(side * rows, width), gu[q], preferred_element_type=F32)
        r = r.reshape(side, rows, 2 * hc)
        for p in range(side):
            at = (mirror[chunk], mirror[p]) if mirrored else (chunk, p)
            i, j = at if t == 0 else at[::-1]
            pre[i, j] += r[p]

    def own_dot(t, chunk):
        project(own, t, t, chunk, False)

    def sib_dot(t, chunk):
        arrived(sib.at[t, chunk], d2d_send.at[t, chunk], d2d_recv.at[t, chunk])
        project(sib, t, 2 + t, chunk, True)

    waiting = []
    loaded = False
    for step in range(side // 2 + nb):
        complete = []
        for t in range(2):
            for d in range(2):
                if 0 < step <= hops[d]:
                    p = pos[side - step if d == 0 else step]
                    arrived(own.at[t, 0, p], p1_send.at[t, p], p1_recv.at[t, p])
                if step < hops[d]:
                    pass_on(t, d, step)
        for h in reversed(range(side // 2 + 1)):
            b = step - h
            if b < 0 or b >= nb:
                continue
            lo, hi = blocks[b]
            for t in range(2):
                if h == 0:
                    for d in range(2):
                        forward(t, d, 0, b)
                    if b == nb - 1:
                        complete.append((t, 0))
                    continue
                for d in range(2):
                    if h > hops[d]:
                        continue
                    chunk = pos[(side - h) % side if d == 0 else h]
                    arrived(own.at[t, chunk, lo:hi], ring_send.at[t, 0, 0, b], ring_recv.at[t, chunk, b])
                    if h < hops[d]:
                        forward(t, d, h, b)
                    if b == nb - 1:
                        complete.append((t, chunk))
        for t, chunk in complete:
            start(remote(own.at[t, chunk], sib.at[t, chunk], d2d_send.at[t, chunk], d2d_recv.at[t, chunk], other))
        if step == 0:
            start(remote(
                down.at[0, :, pl.ds(pl.multiple_of((1 - core) * half, LANES), half)], wd.at[1],
                x_send.at[0], x_recv.at[0], other,
            ))
            pre[...] = jnp.zeros_like(pre)
            for copy in small_loads:
                copy.wait()
            experts = scores.shape[0]
            picked = [
                sum(jnp.where(named[k:k + 1, :] == e, scores[e:e + 1, :], 0.0) for e in range(experts)) for k in range(2)
            ]
            top = jnp.maximum(picked[0], picked[1])
            raised = [jnp.exp(v - top) for v in picked]
            weight = [v / (raised[0] + raised[1]) for v in raised]
            wall[0, 0] = jnp.zeros_like(wall[0, 0])
            for e in range(experts):
                wall[0, 0, :, e * rows:(e + 1) * rows] = sum(
                    jnp.where(named[k:k + 1, :] == e, weight[k], 0.0) for k in range(2)
                )
        if step == nb:
            for k in order[1:]:
                back = pos[side - k]
                start(remote(wall.at[0, 0], wall.at[0, back], w1_send.at[back], w1_recv.at[back], along(0, k)))
        if step == side // 2 + nb - 1:
            for p in range(1, side):
                arrived(wall.at[0, p], w1_send.at[p], w1_recv.at[p])
            for k in order[1:]:
                back = pos[side - k]
                start(remote(wall.at[0], wall.at[back], w2_send.at[back], w2_recv.at[back], along(1, k)))
        if (complete or waiting) and not loaded:
            for copy in loads:
                copy.wait()
            loaded = True
        for t, chunk in complete:
            own_dot(t, chunk)
        for t, chunk in waiting:
            sib_dot(t, chunk)
        waiting = complete
    for t, chunk in waiting:
        sib_dot(t, chunk)

    for i in range(side):
        g, u = pre[i, :, :, :hc], pre[i, :, :, hc:]
        h_here = (g / (1.0 + jnp.exp(-g)) * u).astype(BF16)
        hid[i] = h_here
        for j in range(side):
            hmir[mirror[i], mirror[j]] = h_here[j]
    start(remote(hmir, hsib, x_send.at[1], x_recv.at[1], other))

    for p in range(1, side):
        arrived(wall.at[p], w2_send.at[p], w2_recv.at[p])
    lane = lax.broadcasted_iota(jnp.int32, (side, rows, LANES), 2)
    row = lax.broadcasted_iota(jnp.int32, (side, rows, LANES), 1)
    for i in range(side):
        spread = jnp.broadcast_to(wall[i], (side, rows, LANES))
        wcol[i] = jnp.sum(jnp.where(lane == expert * rows + row, spread, 0.0), axis=2, keepdims=True)

    wd_load.wait()
    arrived(wd.at[1], x_send.at[0], x_recv.at[0])
    arrived(hsib, x_send.at[1], x_recv.at[1])

    def make_part(t, chunk):
        if t == 0:
            a, b, scale = hid[chunk], hsib[chunk], wcol[chunk]
        else:
            a, b, scale = hid[:, chunk], hsib[:, chunk], wcol[:, chunk]
        cols = slice(t * width, (t + 1) * width)
        r = jnp.dot(a.reshape(side * rows, hc), wd[0, :, cols], preferred_element_type=F32)
        r += jnp.dot(b.reshape(side * rows, hc), wd[1, :, cols], preferred_element_type=F32)
        part[t, chunk] = r.reshape(side, rows, width) * scale

    back_blocks = blocks[::-1]
    made = set()

    def need(t, k):
        if (t, k) not in made:
            made.add((t, k))
            make_part(t, pos[k])

    def handled(h):
        return [(t, d, hops[d] - h if d == 0 else side - hops[d] + h) for t in range(2) for d in range(2) if h < hops[d]]

    for h in range(side // 2):
        for b in range(nb):
            lo, hi = back_blocks[b]
            for t, d, k in handled(h):
                need(t, k)
                value = part[t, pos[k], lo:hi]
                if h > 0:
                    arrived(crecv.at[t, d, h, lo:hi], cr_send.at[t, 0, 0, b], cr_recv.at[t, d, h, b])
                    value = value + crecv[t, d, h, lo:hi].astype(F32)
                csend[t, d, h, lo:hi] = value.astype(BF16)
                start(remote(
                    csend.at[t, d, h, lo:hi], crecv.at[t, d, h + 1, lo:hi],
                    cr_send.at[t, d, h, b], cr_recv.at[t, d, h + 1, b], along(1 - t, 1 if d == 0 else side - 1),
                ))
        for t, _, k in handled(h + 1):
            need(t, k)
    for t in range(2):
        need(t, 0)
    for b in range(nb):
        lo, hi = back_blocks[b]
        for t in range(2):
            total = part[t, 0, lo:hi]
            for d in range(2):
                arrived(crecv.at[t, d, hops[d], lo:hi], cr_send.at[t, 0, 0, b], cr_recv.at[t, d, hops[d], b])
                total = total + crecv[t, d, hops[d], lo:hi].astype(F32)
            part[t, 0, lo:hi] = total
            fsend[t, lo:hi] = total.astype(BF16)
            for p in reversed(range(max(lo, 1), hi)):
                back = pos[side - order[p]]
                start(remote(
                    fsend.at[t, p], frecv.at[t, back], f_send.at[t, back], f_recv.at[t, back], along(t, order[p])
                ))
    for t in range(2):
        total = part[t, 0, 0]
        for p in range(1, side):
            arrived(frecv.at[t, p], f_send.at[t, p], f_recv.at[t, p])
            total = total + frecv[t, p].astype(F32)
        out[:, t * width:(t + 1) * width] = total.astype(out.dtype)
    for copy in started:
        copy.wait_send()


def solution(mesh):
    n_expert = mesh.shape["expert"]
    side = math.isqrt(n_expert)
    nb = side // 2 + 1

    def layer(tokens, routes, router_logits, gate_weight, up_weight, down_weight):
        rows, width = tokens.shape[0], tokens.shape[1] // 4
        experts = router_logits.shape[1]
        hc = down_weight.shape[1]
        hop = side // 2
        dma = pltpu.SemaphoreType.DMA
        scratch = [
            pltpu.VMEM((routes.shape[1], rows), jnp.int32),
            pltpu.VMEM((experts, rows), F32),
            pltpu.VMEM((4, width, 2 * hc), BF16),
            pltpu.VMEM((2, hc, 2 * width), BF16),
            pltpu.VMEM((2, side, side, rows, width), BF16),
            pltpu.VMEM((2, side, side, rows, width), BF16),
            pltpu.VMEM((side, side, rows, 2 * hc), F32),
            pltpu.VMEM((side, side, rows, hc), BF16),
            pltpu.VMEM((side, side, rows, hc), BF16),
            pltpu.VMEM((side, side, rows, hc), BF16),
            pltpu.VMEM((side, side, 1, LANES), F32),
            pltpu.VMEM((side, side, rows, 1), F32),
            pltpu.VMEM((2, side, side, rows, width), F32),
            pltpu.VMEM((2, 2, hop, side, rows, width), BF16),
            pltpu.VMEM((2, 2, hop + 1, side, rows, width), BF16),
            pltpu.VMEM((2, side, rows, width), BF16),
            pltpu.VMEM((2, side, rows, width), BF16),
            dma((13,)),
            dma((2, side)), dma((2, side)),
            dma((2, 2, hop, nb)), dma((2, side, nb)),
            dma((2, side)), dma((2, side)),
            dma((side,)), dma((side,)), dma((side,)), dma((side,)),
            dma((2,)), dma((2,)),
            dma((2, 2, hop, nb)), dma((2, 2, hop + 1, nb)),
            dma((2, side)), dma((2, side)),
        ]
        hbm = pl.BlockSpec(memory_space=pl.ANY)
        return pl.pallas_call(
            functools.partial(kernel, side, n_expert // experts),
            out_shape=jax.ShapeDtypeStruct((rows, 2 * width), BF16),
            in_specs=[hbm] * 6,
            out_specs=pl.BlockSpec(memory_space=pltpu.VMEM),
            scratch_shapes=scratch,
            compiler_params=pltpu.CompilerParams(
                collective_id=0, has_side_effects=True, vmem_limit_bytes=60 * 1024 * 1024
            ),
            name="moe_layer",
        )(tokens, routes.T, router_logits.T, gate_weight, up_weight, down_weight)

    return jax.shard_map(
        layer,
        mesh=mesh,
        in_specs=(
            P(("groups", "expert"), None),
            P(("groups", "expert"), None),
            P(("groups", "expert"), None),
            P("expert", None, "tensor"),
            P("expert", None, "tensor"),
            P("expert", "tensor", None),
        ),
        out_specs=P(("groups", "expert"), "tensor"),
        check_vma=False,
    )
```

```python
import functools
import math

import jax
import jax.numpy as jnp
from jax import lax
from jax.experimental import pallas as pl
from jax.experimental.pallas import tpu as pltpu
from jax.sharding import PartitionSpec as P

MESH = pl.DeviceIdType.MESH
F32, BF16 = jnp.float32, jnp.bfloat16
LANES = 128


def ring_order(side):
    order = [0]
    for k in range(1, side // 2):
        order += [k, side - k]
    return order + [side // 2]


def kernel(
    side, segs, tok, routes, logits, gate, up, down, out,
    named, scores, gu, wd, own, sib, pre, hid, hmir, hsib, wall, wcol, part, csend, crecv, fsend, frecv,
    load_sem, p1_send, p1_recv, ring_send, ring_recv, d2d_send, d2d_recv,
    w1_send, w1_recv, w2_send, w2_recv, x_send, x_recv,
    cr_send, cr_recv, f_send, f_recv,
):
    order = ring_order(side)
    pos = {k: p for p, k in enumerate(order)}
    mirror = [pos[(side - k) % side] for k in order]
    cuts = [0, 1] + list(range(3, side - 2, 2)) + [side]
    blocks = list(zip(cuts[:-1], cuts[1:]))
    nb = len(blocks)
    rows, width = own.shape[3], own.shape[4]
    hc = wd.shape[1]
    hops = (side // 2, side // 2 - 1)
    x_pieces = x_send.shape[0] - 1

    core = lax.axis_index("tensor")
    place = lax.axis_index("expert")
    y, x = place // side, lax.rem(place, side)
    expert = place // segs
    sign = 1 - 2 * core

    def along(axis, k):
        step = sign * k + side
        if axis == 0:
            return {"expert": lax.rem(y + step, side) * side + x}
        return {"expert": y * side + lax.rem(x + step, side)}

    def remote(src, dst, send, recv, device):
        return pltpu.make_async_remote_copy(
            src_ref=src, dst_ref=dst, send_sem=send, recv_sem=recv, device_id=device, device_id_type=MESH
        )

    other = {"tensor": 1 - core}
    started = []

    def start(copy):
        copy.start()
        started.append(copy)

    def arrived(ref, send, recv):
        remote(ref, ref, send, recv, other).wait_recv()

    half = 2 * width
    tok_loads = [
        pltpu.make_async_copy(
            tok.at[:, pl.ds(pl.multiple_of(core * half + t * width, LANES), width)], own.at[t, 0, 0], load_sem.at[t]
        )
        for t in range(2)
    ]
    small_loads = [
        pltpu.make_async_copy(routes, named, load_sem.at[2]),
        pltpu.make_async_copy(logits, scores, load_sem.at[12]),
    ]
    for copy in tok_loads + small_loads:
        copy.start()
    loads = []
    for q in range(4):
        who = core if q < 2 else 1 - core
        first = pl.multiple_of(who * half + (q % 2) * width, LANES)
        for i, matrix in enumerate((gate, up)):
            loads.append(
                pltpu.make_async_copy(
                    matrix.at[0, pl.ds(first, width), :], gu.at[q, :, pl.ds(i * hc, hc)], load_sem.at[4 + 2 * q + i]
                )
            )
    for copy in loads:
        copy.start()
    wd_load = pltpu.make_async_copy(
        down.at[0, :, pl.ds(pl.multiple_of(core * half, LANES), half)], wd.at[0], load_sem.at[3]
    )
    wd_load.start()

    barrier = pltpu.get_barrier_semaphore()
    for k in range(1, side):
        for axis in range(2):
            pl.semaphore_signal(barrier, inc=1, device_id=along(axis, k), device_id_type=MESH)
    pl.semaphore_signal(barrier, inc=1, device_id=other, device_id_type=MESH)
    for copy in tok_loads:
        copy.wait()
    pl.semaphore_wait(barrier, 2 * (side - 1) + 1)

    def pass_on(t, k):
        back = pos[side - k]
        start(remote(own.at[t, 0, 0], own.at[t, 0, back], p1_send.at[t, back], p1_recv.at[t, back], along(t, k)))

    def forward(t, d, h, b):
        lo, hi = blocks[b]
        k = (side - h) % side if d == 0 else h
        k_there = (side - h - 1) % side if d == 0 else h + 1
        start(remote(
            own.at[t, pos[k], lo:hi], own.at[t, pos[k_there], lo:hi],
            ring_send.at[t, d, h, b], ring_recv.at[t, pos[k_there], b], along(1 - t, 1 if d == 0 else side - 1),
        ))

    def project(src, t, q, chunk, mirrored):
        r = jnp.dot(src[t, chunk].reshape(side * rows, width), gu[q], preferred_element_type=F32)
        r = r.reshape(side, rows, 2 * hc)
        for p in range(side):
            at = (mirror[chunk], mirror[p]) if mirrored else (chunk, p)
            i, j = at if t == 0 else at[::-1]
            pre[i, j] += r[p]

    def own_dot(t, chunk):
        project(own, t, t, chunk, False)

    def sib_dot(t, chunk):
        for b, (lo, hi) in enumerate(blocks):
            arrived(sib.at[t, chunk, lo:hi], d2d_send.at[t, chunk, b], d2d_recv.at[t, chunk, b])
        project(sib, t, 2 + t, chunk, True)

    waiting = []
    loaded = False
    for h, b in [(h, b) for h in range(side // 2 + 1) for b in range(nb)]:
        step = h * nb + b
        complete, here = [], []
        lo, hi = blocks[b]
        for t in range(2):
            if step == 0:
                pass_on(t, order[1])
                pass_on(t, order[2])
            for d in range(2):
                if h > hops[d]:
                    continue
                chunk = pos[(side - h) % side if d == 0 else h]
                if h > 0:
                    arrived(own.at[t, chunk, lo:hi], ring_send.at[t, 0, 0, b], ring_recv.at[t, chunk, b])
                elif d == 0:
                    for p in range(max(lo, 1), hi):
                        arrived(own.at[t, 0, p], p1_send.at[t, p], p1_recv.at[t, p])
                if h < hops[d]:
                    forward(t, d, h, b)
                if h > 0 or d == 0:
                    here.append((t, chunk, b))
                    if b == nb - 1:
                        complete.append((t, chunk))
            if step == 0:
                for k in order[3:]:
                    pass_on(t, k)
        for t, chunk, b in here:
            lo, hi = blocks[b]
            start(remote(
                own.at[t, chunk, lo:hi], sib.at[t, chunk, lo:hi], d2d_send.at[t, chunk, b], d2d_recv.at[t, chunk, b], other
            ))
        if step < x_pieces:
            span = half // x_pieces
            start(remote(
                down.at[0, :, pl.ds(pl.multiple_of((1 - core) * half + step * span, LANES), span)],
                wd.at[1, :, step * span:(step + 1) * span], x_send.at[step], x_recv.at[step], other,
            ))
        if step == 0:
            pre[...] = jnp.zeros_like(pre)
            for copy in small_loads:
                copy.wait()
            experts = scores.shape[0]
            picked = [
                sum(jnp.where(named[k:k + 1, :] == e, scores[e:e + 1, :], 0.0) for e in range(experts)) for k in range(2)
            ]
            top = jnp.maximum(picked[0], picked[1])
            raised = [jnp.exp(v - top) for v in picked]
            weight = [v / (raised[0] + raised[1]) for v in raised]
            wall[0, 0] = jnp.zeros_like(wall[0, 0])
            for e in range(experts):
                wall[0, 0, :, e * rows:(e + 1) * rows] = sum(
                    jnp.where(named[k:k + 1, :] == e, weight[k], 0.0) for k in range(2)
                )
        if step == nb:
            for k in order[1:]:
                back = pos[side - k]
                start(remote(wall.at[0, 0], wall.at[0, back], w1_send.at[back], w1_recv.at[back], along(0, k)))
        if step == 2 * nb:
            for p in range(1, side):
                arrived(wall.at[0, p], w1_send.at[p], w1_recv.at[p])
            for k in order[1:]:
                back = pos[side - k]
                start(remote(wall.at[0], wall.at[back], w2_send.at[back], w2_recv.at[back], along(1, k)))
        if complete and not loaded:
            for copy in loads:
                copy.wait()
            loaded = True
        for t, chunk in complete:
            own_dot(t, chunk)
        if complete:
            for t, chunk in waiting:
                sib_dot(t, chunk)
            waiting = complete
    for t, chunk in waiting:
        sib_dot(t, chunk)

    for i in range(side):
        g, u = pre[i, :, :, :hc], pre[i, :, :, hc:]
        h_here = (g / (1.0 + jnp.exp(-g)) * u).astype(BF16)
        hid[i] = h_here
        for j in range(side):
            hmir[mirror[i], mirror[j]] = h_here[j]
    start(remote(hmir, hsib, x_send.at[x_pieces], x_recv.at[x_pieces], other))

    for p in range(1, side):
        arrived(wall.at[p], w2_send.at[p], w2_recv.at[p])
    lane = lax.broadcasted_iota(jnp.int32, (side, rows, LANES), 2)
    row = lax.broadcasted_iota(jnp.int32, (side, rows, LANES), 1)
    for i in range(side):
        spread = jnp.broadcast_to(wall[i], (side, rows, LANES))
        wcol[i] = jnp.sum(jnp.where(lane == expert * rows + row, spread, 0.0), axis=2, keepdims=True)

    wd_load.wait()
    for i in range(x_pieces):
        span = half // x_pieces
        arrived(wd.at[1, :, i * span:(i + 1) * span], x_send.at[i], x_recv.at[i])
    arrived(hsib, x_send.at[x_pieces], x_recv.at[x_pieces])

    def make_part(t, chunk):
        if t == 0:
            a, b, scale = hid[chunk], hsib[chunk], wcol[chunk]
        else:
            a, b, scale = hid[:, chunk], hsib[:, chunk], wcol[:, chunk]
        cols = slice(t * width, (t + 1) * width)
        r = jnp.dot(a.reshape(side * rows, hc), wd[0, :, cols], preferred_element_type=F32)
        r += jnp.dot(b.reshape(side * rows, hc), wd[1, :, cols], preferred_element_type=F32)
        part[t, chunk] = r.reshape(side, rows, width) * scale

    back_blocks = blocks[::-1]
    made = set()

    def need(t, k):
        if (t, k) not in made:
            made.add((t, k))
            make_part(t, pos[k])

    def handled(h):
        return [(t, d, hops[d] - h if d == 0 else side - hops[d] + h) for t in range(2) for d in range(2) if h < hops[d]]

    for h in range(side // 2):
        for b in range(nb):
            lo, hi = back_blocks[b]
            for t, d, k in handled(h):
                need(t, k)
                value = part[t, pos[k], lo:hi]
                if h > 0:
                    arrived(crecv.at[t, d, h, lo:hi], cr_send.at[t, 0, 0, b], cr_recv.at[t, d, h, b])
                    value = value + crecv[t, d, h, lo:hi].astype(F32)
                csend[t, d, h, lo:hi] = value.astype(BF16)
                start(remote(
                    csend.at[t, d, h, lo:hi], crecv.at[t, d, h + 1, lo:hi],
                    cr_send.at[t, d, h, b], cr_recv.at[t, d, h + 1, b], along(1 - t, 1 if d == 0 else side - 1),
                ))
        for t, _, k in handled(h + 1):
            need(t, k)
    for t in range(2):
        need(t, 0)
    for b in range(nb):
        lo, hi = back_blocks[b]
        for t in range(2):
            total = part[t, 0, lo:hi]
            for d in range(2):
                arrived(crecv.at[t, d, hops[d], lo:hi], cr_send.at[t, 0, 0, b], cr_recv.at[t, d, hops[d], b])
                total = total + crecv[t, d, hops[d], lo:hi].astype(F32)
            part[t, 0, lo:hi] = total
            fsend[t, lo:hi] = total.astype(BF16)
            for p in reversed(range(max(lo, 1), hi)):
                back = pos[side - order[p]]
                start(remote(
                    fsend.at[t, p], frecv.at[t, back], f_send.at[t, back], f_recv.at[t, back], along(t, order[p])
                ))
    for t in range(2):
        total = part[t, 0, 0]
        for p in range(1, side):
            arrived(frecv.at[t, p], f_send.at[t, p], f_recv.at[t, p])
            total = total + frecv[t, p].astype(F32)
        out[:, t * width:(t + 1) * width] = total.astype(out.dtype)
    for copy in started:
        copy.wait_send()


def solution(mesh):
    n_expert = mesh.shape["expert"]
    side = math.isqrt(n_expert)
    nb = len([0, 1] + list(range(3, side - 2, 2)))

    def layer(tokens, routes, router_logits, gate_weight, up_weight, down_weight):
        rows, width = tokens.shape[0], tokens.shape[1] // 4
        experts = router_logits.shape[1]
        hc = down_weight.shape[1]
        hop = side // 2
        pieces = math.gcd(2 * width // LANES, side)
        dma = pltpu.SemaphoreType.DMA
        scratch = [
            pltpu.VMEM((routes.shape[1], rows), jnp.int32),
            pltpu.VMEM((experts, rows), F32),
            pltpu.VMEM((4, width, 2 * hc), BF16),
            pltpu.VMEM((2, hc, 2 * width), BF16),
            pltpu.VMEM((2, side, side, rows, width), BF16),
            pltpu.VMEM((2, side, side, rows, width), BF16),
            pltpu.VMEM((side, side, rows, 2 * hc), F32),
            pltpu.VMEM((side, side, rows, hc), BF16),
            pltpu.VMEM((side, side, rows, hc), BF16),
            pltpu.VMEM((side, side, rows, hc), BF16),
            pltpu.VMEM((side, side, 1, LANES), F32),
            pltpu.VMEM((side, side, rows, 1), F32),
            pltpu.VMEM((2, side, side, rows, width), F32),
            pltpu.VMEM((2, 2, hop, side, rows, width), BF16),
            pltpu.VMEM((2, 2, hop + 1, side, rows, width), BF16),
            pltpu.VMEM((2, side, rows, width), BF16),
            pltpu.VMEM((2, side, rows, width), BF16),
            dma((13,)),
            dma((2, side)), dma((2, side)),
            dma((2, 2, hop, nb)), dma((2, side, nb)),
            dma((2, side, nb)), dma((2, side, nb)),
            dma((side,)), dma((side,)), dma((side,)), dma((side,)),
            dma((pieces + 1,)), dma((pieces + 1,)),
            dma((2, 2, hop, nb)), dma((2, 2, hop + 1, nb)),
            dma((2, side)), dma((2, side)),
        ]
        hbm = pl.BlockSpec(memory_space=pl.ANY)
        return pl.pallas_call(
            functools.partial(kernel, side, n_expert // experts),
            out_shape=jax.ShapeDtypeStruct((rows, 2 * width), BF16),
            in_specs=[hbm] * 6,
            out_specs=pl.BlockSpec(memory_space=pltpu.VMEM),
            scratch_shapes=scratch,
            compiler_params=pltpu.CompilerParams(
                collective_id=0, has_side_effects=True, vmem_limit_bytes=60 * 1024 * 1024
            ),
            name="moe_layer",
        )(tokens, routes.T, router_logits.T, gate_weight, up_weight, down_weight)

    return jax.shard_map(
        layer,
        mesh=mesh,
        in_specs=(
            P(("groups", "expert"), None),
            P(("groups", "expert"), None),
            P(("groups", "expert"), None),
            P("expert", None, "tensor"),
            P("expert", None, "tensor"),
            P("expert", "tensor", None),
        ),
        out_specs=P(("groups", "expert"), "tensor"),
        check_vma=False,
    )
```

```python
import functools
import math

import jax
import jax.numpy as jnp
from jax import lax
from jax.experimental import pallas as pl
from jax.experimental.pallas import tpu as pltpu
from jax.sharding import PartitionSpec as P

MESH = pl.DeviceIdType.MESH
F32, BF16 = jnp.float32, jnp.bfloat16
LANES = 128


def ring_order(side):
    order = [0]
    for k in range(1, side // 2):
        order += [k, side - k]
    return order + [side // 2]


def kernel(
    side, segs, tok, routes, logits, gate, up, down, out,
    named, scores, gu, wd, own, sib, pre, hid, hmir, wall, wcol, part, csend, crecv, fsend, frecv,
    load_sem, p1_send, p1_recv, ring_send, ring_recv, d2d_send, d2d_recv,
    w1_send, w1_recv, w2_send, w2_recv, x_send, x_recv,
    cr_send, cr_recv, f_send, f_recv,
):
    order = ring_order(side)
    pos = {k: p for p, k in enumerate(order)}
    mirror = [pos[(side - k) % side] for k in order]
    cuts = [0, 1] + list(range(3, side - 2, 2)) + [side]
    blocks = list(zip(cuts[:-1], cuts[1:]))
    nb = len(blocks)
    rows, width = own.shape[3], own.shape[4]
    hc = wd.shape[0] // 2
    hops = (side // 2, side // 2 - 1)
    x_pieces = x_send.shape[0] - 1

    core = lax.axis_index("tensor")
    place = lax.axis_index("expert")
    y, x = place // side, lax.rem(place, side)
    expert = place // segs
    sign = 1 - 2 * core

    def along(axis, k):
        step = sign * k + side
        if axis == 0:
            return {"expert": lax.rem(y + step, side) * side + x}
        return {"expert": y * side + lax.rem(x + step, side)}

    def remote(src, dst, send, recv, device):
        return pltpu.make_async_remote_copy(
            src_ref=src, dst_ref=dst, send_sem=send, recv_sem=recv, device_id=device, device_id_type=MESH
        )

    other = {"tensor": 1 - core}
    started = []

    def start(copy):
        copy.start()
        started.append(copy)

    def arrived(ref, send, recv):
        remote(ref, ref, send, recv, other).wait_recv()

    half = 2 * width
    tok_loads = [
        pltpu.make_async_copy(
            tok.at[:, pl.ds(pl.multiple_of(core * half + t * width, LANES), width)], own.at[t, 0, 0], load_sem.at[t]
        )
        for t in range(2)
    ]
    small_loads = [
        pltpu.make_async_copy(routes, named, load_sem.at[2]),
        pltpu.make_async_copy(logits, scores, load_sem.at[12]),
    ]
    for copy in tok_loads + small_loads:
        copy.start()
    loads = []
    for q in range(4):
        who = core if q < 2 else 1 - core
        first = pl.multiple_of(who * half + (q % 2) * width, LANES)
        for i, matrix in enumerate((gate, up)):
            loads.append(
                pltpu.make_async_copy(
                    matrix.at[0, pl.ds(first, width), :], gu.at[q, :, pl.ds(i * hc, hc)], load_sem.at[4 + 2 * q + i]
                )
            )
    for copy in loads:
        copy.start()
    wd_load = pltpu.make_async_copy(
        down.at[0, :, pl.ds(pl.multiple_of(core * half, LANES), half)], wd.at[:hc], load_sem.at[3]
    )
    wd_load.start()

    barrier = pltpu.get_barrier_semaphore()
    for k in range(1, side):
        for axis in range(2):
            pl.semaphore_signal(barrier, inc=1, device_id=along(axis, k), device_id_type=MESH)
    pl.semaphore_signal(barrier, inc=1, device_id=other, device_id_type=MESH)
    for copy in tok_loads:
        copy.wait()
    pl.semaphore_wait(barrier, 2 * (side - 1) + 1)

    def pass_on(t, k):
        back = pos[side - k]
        start(remote(own.at[t, 0, 0], own.at[t, 0, back], p1_send.at[t, back], p1_recv.at[t, back], along(t, k)))

    def forward(t, d, h, b):
        lo, hi = blocks[b]
        k = (side - h) % side if d == 0 else h
        k_there = (side - h - 1) % side if d == 0 else h + 1
        start(remote(
            own.at[t, pos[k], lo:hi], own.at[t, pos[k_there], lo:hi],
            ring_send.at[t, d, h, b], ring_recv.at[t, pos[k_there], b], along(1 - t, 1 if d == 0 else side - 1),
        ))

    def span_of(h):
        return (0, 1) if h == 0 else (2 * h - 1, min(2 * h + 1, side))

    def project(src, t, q, h, mirrored):
        first, last = span_of(h)
        r = jnp.dot(src[t, first:last].reshape((last - first) * side * rows, width), gu[q], preferred_element_type=F32)
        r = r.reshape(last - first, side, rows, 2 * hc)
        for c in range(first, last):
            for p in range(side):
                at = (mirror[c], mirror[p]) if mirrored else (c, p)
                i, j = at if t == 0 else at[::-1]
                pre[i, j] += r[c - first, p]

    def own_dots(h):
        for t in range(2):
            project(own, t, t, h, False)

    def sib_dots(h):
        for t in range(2):
            for chunk in range(*span_of(h)):
                for b, (lo, hi) in enumerate(blocks):
                    arrived(sib.at[t, chunk, lo:hi], d2d_send.at[t, chunk, b], d2d_recv.at[t, chunk, b])
            project(sib, t, 2 + t, h, True)

    for h, b in [(h, b) for h in range(side // 2 + 1) for b in range(nb)]:
        step = h * nb + b
        here = []
        lo, hi = blocks[b]
        for t in range(2):
            if step == 0:
                pass_on(t, order[1])
                pass_on(t, order[2])
            for d in range(2):
                if h > hops[d]:
                    continue
                chunk = pos[(side - h) % side if d == 0 else h]
                if h > 0:
                    arrived(own.at[t, chunk, lo:hi], ring_send.at[t, 0, 0, b], ring_recv.at[t, chunk, b])
                elif d == 0:
                    for p in range(max(lo, 1), hi):
                        arrived(own.at[t, 0, p], p1_send.at[t, p], p1_recv.at[t, p])
                if h < hops[d]:
                    forward(t, d, h, b)
                if h > 0 or d == 0:
                    here.append((t, chunk, b))
            if step == 0:
                for k in order[3:]:
                    pass_on(t, k)
        for t, chunk, b in here:
            lo, hi = blocks[b]
            start(remote(
                own.at[t, chunk, lo:hi], sib.at[t, chunk, lo:hi], d2d_send.at[t, chunk, b], d2d_recv.at[t, chunk, b], other
            ))
        if step < x_pieces:
            span = half // x_pieces
            start(remote(
                down.at[0, :, pl.ds(pl.multiple_of((1 - core) * half + step * span, LANES), span)],
                wd.at[hc:, step * span:(step + 1) * span], x_send.at[step], x_recv.at[step], other,
            ))
        if step == 0:
            pre[...] = jnp.zeros_like(pre)
            for copy in small_loads:
                copy.wait()
            experts = scores.shape[0]
            picked = [
                sum(jnp.where(named[k:k + 1, :] == e, scores[e:e + 1, :], 0.0) for e in range(experts)) for k in range(2)
            ]
            top = jnp.maximum(picked[0], picked[1])
            raised = [jnp.exp(v - top) for v in picked]
            weight = [v / (raised[0] + raised[1]) for v in raised]
            wall[0, 0] = jnp.zeros_like(wall[0, 0])
            for e in range(experts):
                wall[0, 0, :, e * rows:(e + 1) * rows] = sum(
                    jnp.where(named[k:k + 1, :] == e, weight[k], 0.0) for k in range(2)
                )
        if step == nb:
            for k in order[1:]:
                back = pos[side - k]
                start(remote(wall.at[0, 0], wall.at[0, back], w1_send.at[back], w1_recv.at[back], along(0, k)))
        if step == 2 * nb:
            for p in range(1, side):
                arrived(wall.at[0, p], w1_send.at[p], w1_recv.at[p])
            for k in order[1:]:
                back = pos[side - k]
                start(remote(wall.at[0], wall.at[back], w2_send.at[back], w2_recv.at[back], along(1, k)))
        if step == nb - 1:
            for copy in loads:
                copy.wait()
        if b == nb - 1:
            own_dots(h)
        if b == 1 and h > 0:
            sib_dots(h - 1)
    sib_dots(side // 2)

    for i in range(side):
        g, u = pre[i, :, :, :hc], pre[i, :, :, hc:]
        h_here = (g / (1.0 + jnp.exp(-g)) * u).astype(BF16)
        hid[i, :, :, :hc] = h_here
        for j in range(side):
            hmir[mirror[i], mirror[j]] = h_here[j]
    start(remote(hmir, hid.at[:, :, :, hc:], x_send.at[x_pieces], x_recv.at[x_pieces], other))

    for p in range(1, side):
        arrived(wall.at[p], w2_send.at[p], w2_recv.at[p])
    lane = lax.broadcasted_iota(jnp.int32, (side, rows, LANES), 2)
    row = lax.broadcasted_iota(jnp.int32, (side, rows, LANES), 1)
    for i in range(side):
        spread = jnp.broadcast_to(wall[i], (side, rows, LANES))
        wcol[i] = jnp.sum(jnp.where(lane == expert * rows + row, spread, 0.0), axis=2, keepdims=True)

    wd_load.wait()
    for i in range(x_pieces):
        span = half // x_pieces
        arrived(wd.at[hc:, i * span:(i + 1) * span], x_send.at[i], x_recv.at[i])
    arrived(hid.at[:, :, :, hc:], x_send.at[x_pieces], x_recv.at[x_pieces])

    def make_parts(t, first):
        a = hid[first:first + 2] if t == 0 else hid[:, first:first + 2]
        r = jnp.dot(
            a.reshape(2 * side * rows, 2 * hc), wd[:, t * width:(t + 1) * width], preferred_element_type=F32
        )
        if t == 0:
            part[t, first:first + 2] = r.reshape(2, side, rows, width) * wcol[first:first + 2]
        else:
            r = r.reshape(side, 2, rows, width)
            for c in range(2):
                part[t, first + c] = r[:, c] * wcol[:, first + c]

    back_blocks = blocks[::-1]
    for h in range(side // 2):
        first = side - 2 - 2 * h
        halves = [(t, b) for t in range(2) for b in range(nb)] if h == 0 else [(t, b) for b in range(nb) for t in range(2)]
        for t, b in halves:
            if h == 0 and b == 0:
                make_parts(t, first)
            lo, hi = back_blocks[b]
            for d in range(2):
                if h >= hops[d]:
                    continue
                k = hops[d] - h if d == 0 else side - hops[d] + h
                value = part[t, pos[k], lo:hi]
                if h > 0:
                    arrived(crecv.at[t, d, h, lo:hi], cr_send.at[t, 0, 0, b], cr_recv.at[t, d, h, b])
                    value = value + crecv[t, d, h, lo:hi].astype(F32)
                csend[t, d, h, lo:hi] = value.astype(BF16)
                start(remote(
                    csend.at[t, d, h, lo:hi], crecv.at[t, d, h + 1, lo:hi],
                    cr_send.at[t, d, h, b], cr_recv.at[t, d, h + 1, b], along(1 - t, 1 if d == 0 else side - 1),
                ))
        if h + 1 < side // 2:
            for t in range(2):
                make_parts(t, first - 2)
    for b in range(nb):
        lo, hi = back_blocks[b]
        for t in range(2):
            total = part[t, 0, lo:hi]
            for d in range(2):
                arrived(crecv.at[t, d, hops[d], lo:hi], cr_send.at[t, 0, 0, b], cr_recv.at[t, d, hops[d], b])
                total = total + crecv[t, d, hops[d], lo:hi].astype(F32)
            part[t, 0, lo:hi] = total
            fsend[t, lo:hi] = total.astype(BF16)
            for p in reversed(range(max(lo, 1), hi)):
                back = pos[side - order[p]]
                start(remote(
                    fsend.at[t, p], frecv.at[t, back], f_send.at[t, back], f_recv.at[t, back], along(t, order[p])
                ))
    for t in range(2):
        total = part[t, 0, 0]
        for p in range(1, side):
            arrived(frecv.at[t, p], f_send.at[t, p], f_recv.at[t, p])
            total = total + frecv[t, p].astype(F32)
        out[:, t * width:(t + 1) * width] = total.astype(out.dtype)
    for copy in started:
        copy.wait_send()


def solution(mesh):
    n_expert = mesh.shape["expert"]
    side = math.isqrt(n_expert)
    nb = len([0, 1] + list(range(3, side - 2, 2)))

    def layer(tokens, routes, router_logits, gate_weight, up_weight, down_weight):
        rows, width = tokens.shape[0], tokens.shape[1] // 4
        experts = router_logits.shape[1]
        hc = down_weight.shape[1]
        hop = side // 2
        pieces = math.gcd(2 * width // LANES, side)
        dma = pltpu.SemaphoreType.DMA
        scratch = [
            pltpu.VMEM((routes.shape[1], rows), jnp.int32),
            pltpu.VMEM((experts, rows), F32),
            pltpu.VMEM((4, width, 2 * hc), BF16),
            pltpu.VMEM((2 * hc, 2 * width), BF16),
            pltpu.VMEM((2, side, side, rows, width), BF16),
            pltpu.VMEM((2, side, side, rows, width), BF16),
            pltpu.VMEM((side, side, rows, 2 * hc), F32),
            pltpu.VMEM((side, side, rows, 2 * hc), BF16),
            pltpu.VMEM((side, side, rows, hc), BF16),
            pltpu.VMEM((side, side, 1, LANES), F32),
            pltpu.VMEM((side, side, rows, 1), F32),
            pltpu.VMEM((2, side, side, rows, width), F32),
            pltpu.VMEM((2, 2, hop, side, rows, width), BF16),
            pltpu.VMEM((2, 2, hop + 1, side, rows, width), BF16),
            pltpu.VMEM((2, side, rows, width), BF16),
            pltpu.VMEM((2, side, rows, width), BF16),
            dma((13,)),
            dma((2, side)), dma((2, side)),
            dma((2, 2, hop, nb)), dma((2, side, nb)),
            dma((2, side, nb)), dma((2, side, nb)),
            dma((side,)), dma((side,)), dma((side,)), dma((side,)),
            dma((pieces + 1,)), dma((pieces + 1,)),
            dma((2, 2, hop, nb)), dma((2, 2, hop + 1, nb)),
            dma((2, side)), dma((2, side)),
        ]
        hbm = pl.BlockSpec(memory_space=pl.ANY)
        return pl.pallas_call(
            functools.partial(kernel, side, n_expert // experts),
            out_shape=jax.ShapeDtypeStruct((rows, 2 * width), BF16),
            in_specs=[hbm] * 6,
            out_specs=pl.BlockSpec(memory_space=pltpu.VMEM),
            scratch_shapes=scratch,
            compiler_params=pltpu.CompilerParams(
                collective_id=0, has_side_effects=True, vmem_limit_bytes=60 * 1024 * 1024
            ),
            name="moe_layer",
        )(tokens, routes.T, router_logits.T, gate_weight, up_weight, down_weight)

    return jax.shard_map(
        layer,
        mesh=mesh,
        in_specs=(
            P(("groups", "expert"), None),
            P(("groups", "expert"), None),
            P(("groups", "expert"), None),
            P("expert", None, "tensor"),
            P("expert", None, "tensor"),
            P("expert", "tensor", None),
        ),
        out_specs=P(("groups", "expert"), "tensor"),
        check_vma=False,
    )
```

```python
import functools
import math

import jax
import jax.numpy as jnp
from jax import lax
from jax.experimental import pallas as pl
from jax.experimental.pallas import tpu as pltpu
from jax.sharding import PartitionSpec as P

MESH = pl.DeviceIdType.MESH
F32, BF16 = jnp.float32, jnp.bfloat16
LANES = 128


def ring_order(side):
    order = [0]
    for k in range(1, side // 2):
        order += [k, side - k]
    return order + [side // 2]


def kernel(
    side, segs, tok, routes, logits, gate, up, down, out,
    named, scores, gu, wd, own, sib, pre, hid, hmir, wall, wcol, part, csend, crecv, fsend, frecv,
    load_sem, p1_send, p1_recv, ring_send, ring_recv, d2d_send, d2d_recv,
    w1_send, w1_recv, w2_send, w2_recv, x_send, x_recv,
    cr_send, cr_recv, f_send, f_recv,
):
    order = ring_order(side)
    pos = {k: p for p, k in enumerate(order)}
    mirror = [pos[(side - k) % side] for k in order]
    cuts = [0, 1] + list(range(3, side - 2, 2)) + [side]
    blocks = list(zip(cuts[:-1], cuts[1:]))
    nb = len(blocks)
    rows, width = own.shape[3], own.shape[4]
    hc = wd.shape[0] // 2
    hops = (side // 2, side // 2 - 1)
    x_pieces = x_send.shape[0] - side

    core = lax.axis_index("tensor")
    place = lax.axis_index("expert")
    y, x = place // side, lax.rem(place, side)
    expert = place // segs
    sign = 1 - 2 * core

    def along(axis, k):
        step = sign * k + side
        if axis == 0:
            return {"expert": lax.rem(y + step, side) * side + x}
        return {"expert": y * side + lax.rem(x + step, side)}

    def remote(src, dst, send, recv, device):
        return pltpu.make_async_remote_copy(
            src_ref=src, dst_ref=dst, send_sem=send, recv_sem=recv, device_id=device, device_id_type=MESH
        )

    other = {"tensor": 1 - core}
    started = []

    def start(copy):
        copy.start()
        started.append(copy)

    def arrived(ref, send, recv):
        remote(ref, ref, send, recv, other).wait_recv()

    half = 2 * width
    tok_loads = [
        pltpu.make_async_copy(
            tok.at[:, pl.ds(pl.multiple_of(core * half + t * width, LANES), width)], own.at[t, 0, 0], load_sem.at[t]
        )
        for t in range(2)
    ]
    small_loads = [
        pltpu.make_async_copy(routes, named, load_sem.at[2]),
        pltpu.make_async_copy(logits, scores, load_sem.at[12]),
    ]
    for copy in tok_loads + small_loads:
        copy.start()
    loads = []
    for q in range(4):
        who = core if q < 2 else 1 - core
        first = pl.multiple_of(who * half + (q % 2) * width, LANES)
        for i, matrix in enumerate((gate, up)):
            loads.append(
                pltpu.make_async_copy(
                    matrix.at[0, pl.ds(first, width), :], gu.at[q, :, pl.ds(i * hc, hc)], load_sem.at[4 + 2 * q + i]
                )
            )
    wd_load = pltpu.make_async_copy(
        down.at[0, :, pl.ds(pl.multiple_of(core * half, LANES), half)], wd.at[:hc], load_sem.at[3]
    )
    wd_load.start()

    barrier = pltpu.get_barrier_semaphore()
    for k in range(1, side):
        for axis in range(2):
            pl.semaphore_signal(barrier, inc=1, device_id=along(axis, k), device_id_type=MESH)
    pl.semaphore_signal(barrier, inc=1, device_id=other, device_id_type=MESH)
    for copy in tok_loads:
        copy.wait()
    pl.semaphore_wait(barrier, 2 * (side - 1) + 1)

    def pass_on(t, k):
        back = pos[side - k]
        start(remote(own.at[t, 0, 0], own.at[t, 0, back], p1_send.at[t, back], p1_recv.at[t, back], along(t, k)))

    def forward(t, d, h, b):
        lo, hi = blocks[b]
        k = (side - h) % side if d == 0 else h
        k_there = (side - h - 1) % side if d == 0 else h + 1
        start(remote(
            own.at[t, pos[k], lo:hi], own.at[t, pos[k_there], lo:hi],
            ring_send.at[t, d, h, b], ring_recv.at[t, pos[k_there], b], along(1 - t, 1 if d == 0 else side - 1),
        ))

    def span_of(h):
        return (0, 1) if h == 0 else (2 * h - 1, min(2 * h + 1, side))

    def project(src, t, q, h, mirrored):
        first, last = span_of(h)
        r = jnp.dot(src[t, first:last].reshape((last - first) * side * rows, width), gu[q], preferred_element_type=F32)
        r = r.reshape(last - first, side, rows, 2 * hc)
        for c in range(first, last):
            for p in range(side):
                at = (mirror[c], mirror[p]) if mirrored else (c, p)
                i, j = at if t == 0 else at[::-1]
                pre[i, j] += r[c - first, p]

    def own_dots(h):
        for t in range(2):
            project(own, t, t, h, False)

    def sib_dots(h):
        for t in range(2):
            for chunk in range(*span_of(h)):
                for b, (lo, hi) in enumerate(blocks):
                    arrived(sib.at[t, chunk, lo:hi], d2d_send.at[t, chunk, b], d2d_recv.at[t, chunk, b])
            project(sib, t, 2 + t, h, True)

    for h, b in [(h, b) for h in range(side // 2 + 1) for b in range(nb)]:
        step = h * nb + b
        here = []
        lo, hi = blocks[b]
        for t in range(2):
            if step == 0:
                pass_on(t, order[1])
                pass_on(t, order[2])
            for d in range(2):
                if h > hops[d]:
                    continue
                chunk = pos[(side - h) % side if d == 0 else h]
                if h > 0:
                    arrived(own.at[t, chunk, lo:hi], ring_send.at[t, 0, 0, b], ring_recv.at[t, chunk, b])
                elif d == 0:
                    for p in range(max(lo, 1), hi):
                        arrived(own.at[t, 0, p], p1_send.at[t, p], p1_recv.at[t, p])
                if h < hops[d]:
                    forward(t, d, h, b)
                if h > 0 or d == 0:
                    here.append((t, chunk, b))
            if step == 0:
                for k in order[3:]:
                    pass_on(t, k)
        for t, chunk, b in here:
            lo, hi = blocks[b]
            start(remote(
                own.at[t, chunk, lo:hi], sib.at[t, chunk, lo:hi], d2d_send.at[t, chunk, b], d2d_recv.at[t, chunk, b], other
            ))
        if step < x_pieces:
            span = half // x_pieces
            start(remote(
                down.at[0, :, pl.ds(pl.multiple_of((1 - core) * half + step * span, LANES), span)],
                wd.at[hc:, step * span:(step + 1) * span], x_send.at[step], x_recv.at[step], other,
            ))
        if step == 0:
            for copy in loads:
                copy.start()
            pre[...] = jnp.zeros_like(pre)
            for copy in small_loads:
                copy.wait()
            experts = scores.shape[0]
            picked = [
                sum(jnp.where(named[k:k + 1, :] == e, scores[e:e + 1, :], 0.0) for e in range(experts)) for k in range(2)
            ]
            top = jnp.maximum(picked[0], picked[1])
            raised = [jnp.exp(v - top) for v in picked]
            weight = [v / (raised[0] + raised[1]) for v in raised]
            wall[0, 0] = jnp.zeros_like(wall[0, 0])
            for e in range(experts):
                wall[0, 0, :, e * rows:(e + 1) * rows] = sum(
                    jnp.where(named[k:k + 1, :] == e, weight[k], 0.0) for k in range(2)
                )
        if step == nb:
            for k in order[1:]:
                back = pos[side - k]
                start(remote(wall.at[0, 0], wall.at[0, back], w1_send.at[back], w1_recv.at[back], along(0, k)))
        if step == 2 * nb:
            for p in range(1, side):
                arrived(wall.at[0, p], w1_send.at[p], w1_recv.at[p])
            for k in order[1:]:
                back = pos[side - k]
                start(remote(wall.at[0], wall.at[back], w2_send.at[back], w2_recv.at[back], along(1, k)))
        if h == 1 and b == 1:
            for copy in loads:
                copy.wait()
        if h > 0 and b == 1:
            own_dots(h - 1)
        if h > 0 and b == min(2, nb - 1):
            sib_dots(h - 1)
    own_dots(side // 2)
    sib_dots(side // 2)

    for i in reversed(range(side)):
        g, u = pre[i, :, :, :hc], pre[i, :, :, hc:]
        h_here = (g / (1.0 + jnp.exp(-g)) * u).astype(BF16)
        hid[i, :, :, :hc] = h_here
        for j in range(side):
            hmir[mirror[i], mirror[j]] = h_here[j]
        m = mirror[i]
        start(remote(hmir.at[m], hid.at[m, :, :, hc:], x_send.at[x_pieces + m], x_recv.at[x_pieces + m], other))

    def other_hidden(first, last):
        for i in range(first, last):
            arrived(hid.at[i, :, :, hc:], x_send.at[x_pieces + i], x_recv.at[x_pieces + i])

    for p in range(1, side):
        arrived(wall.at[p], w2_send.at[p], w2_recv.at[p])
    lane = lax.broadcasted_iota(jnp.int32, (side, rows, LANES), 2)
    row = lax.broadcasted_iota(jnp.int32, (side, rows, LANES), 1)
    for i in range(side):
        spread = jnp.broadcast_to(wall[i], (side, rows, LANES))
        wcol[i] = jnp.sum(jnp.where(lane == expert * rows + row, spread, 0.0), axis=2, keepdims=True)

    wd_load.wait()
    for i in range(x_pieces):
        span = half // x_pieces
        arrived(wd.at[hc:, i * span:(i + 1) * span], x_send.at[i], x_recv.at[i])

    def make_parts(t, first):
        a = hid[first:first + 2] if t == 0 else hid[:, first:first + 2]
        r = jnp.dot(
            a.reshape(2 * side * rows, 2 * hc), wd[:, t * width:(t + 1) * width], preferred_element_type=F32
        )
        if t == 0:
            part[t, first:first + 2] = r.reshape(2, side, rows, width) * wcol[first:first + 2]
        else:
            r = r.reshape(side, 2, rows, width)
            for c in range(2):
                part[t, first + c] = r[:, c] * wcol[:, first + c]

    back_blocks = blocks[::-1]
    for h in range(side // 2):
        first = side - 2 - 2 * h
        halves = [(t, b) for t in range(2) for b in range(nb)] if h == 0 else [(t, b) for b in range(nb) for t in range(2)]
        for t, b in halves:
            if h == 0 and b == 0:
                other_hidden(*((first, side) if t == 0 else (0, first)))
                make_parts(t, first)
            lo, hi = back_blocks[b]
            for d in range(2):
                if h >= hops[d]:
                    continue
                k = hops[d] - h if d == 0 else side - hops[d] + h
                value = part[t, pos[k], lo:hi]
                if h > 0:
                    arrived(crecv.at[t, d, h, lo:hi], cr_send.at[t, 0, 0, b], cr_recv.at[t, d, h, b])
                    value = value + crecv[t, d, h, lo:hi].astype(F32)
                csend[t, d, h, lo:hi] = value.astype(BF16)
                start(remote(
                    csend.at[t, d, h, lo:hi], crecv.at[t, d, h + 1, lo:hi],
                    cr_send.at[t, d, h, b], cr_recv.at[t, d, h + 1, b], along(1 - t, 1 if d == 0 else side - 1),
                ))
        if h + 1 < side // 2:
            for t in range(2):
                make_parts(t, first - 2)
    for b in range(nb):
        lo, hi = back_blocks[b]
        for t in range(2):
            total = part[t, 0, lo:hi]
            for d in range(2):
                arrived(crecv.at[t, d, hops[d], lo:hi], cr_send.at[t, 0, 0, b], cr_recv.at[t, d, hops[d], b])
                total = total + crecv[t, d, hops[d], lo:hi].astype(F32)
            part[t, 0, lo:hi] = total
            fsend[t, lo:hi] = total.astype(BF16)
            for p in reversed(range(max(lo, 1), hi)):
                back = pos[side - order[p]]
                start(remote(
                    fsend.at[t, p], frecv.at[t, back], f_send.at[t, back], f_recv.at[t, back], along(t, order[p])
                ))
    for t in range(2):
        total = part[t, 0, 0]
        for p in range(1, side):
            arrived(frecv.at[t, p], f_send.at[t, p], f_recv.at[t, p])
            total = total + frecv[t, p].astype(F32)
        out[:, t * width:(t + 1) * width] = total.astype(out.dtype)
    for copy in started:
        copy.wait_send()


def solution(mesh):
    n_expert = mesh.shape["expert"]
    side = math.isqrt(n_expert)
    nb = len([0, 1] + list(range(3, side - 2, 2)))

    def layer(tokens, routes, router_logits, gate_weight, up_weight, down_weight):
        rows, width = tokens.shape[0], tokens.shape[1] // 4
        experts = router_logits.shape[1]
        hc = down_weight.shape[1]
        hop = side // 2
        pieces = math.gcd(2 * width // LANES, side)
        dma = pltpu.SemaphoreType.DMA
        scratch = [
            pltpu.VMEM((routes.shape[1], rows), jnp.int32),
            pltpu.VMEM((experts, rows), F32),
            pltpu.VMEM((4, width, 2 * hc), BF16),
            pltpu.VMEM((2 * hc, 2 * width), BF16),
            pltpu.VMEM((2, side, side, rows, width), BF16),
            pltpu.VMEM((2, side, side, rows, width), BF16),
            pltpu.VMEM((side, side, rows, 2 * hc), F32),
            pltpu.VMEM((side, side, rows, 2 * hc), BF16),
            pltpu.VMEM((side, side, rows, hc), BF16),
            pltpu.VMEM((side, side, 1, LANES), F32),
            pltpu.VMEM((side, side, rows, 1), F32),
            pltpu.VMEM((2, side, side, rows, width), F32),
            pltpu.VMEM((2, 2, hop, side, rows, width), BF16),
            pltpu.VMEM((2, 2, hop + 1, side, rows, width), BF16),
            pltpu.VMEM((2, side, rows, width), BF16),
            pltpu.VMEM((2, side, rows, width), BF16),
            dma((13,)),
            dma((2, side)), dma((2, side)),
            dma((2, 2, hop, nb)), dma((2, side, nb)),
            dma((2, side, nb)), dma((2, side, nb)),
            dma((side,)), dma((side,)), dma((side,)), dma((side,)),
            dma((pieces + side,)), dma((pieces + side,)),
            dma((2, 2, hop, nb)), dma((2, 2, hop + 1, nb)),
            dma((2, side)), dma((2, side)),
        ]
        hbm = pl.BlockSpec(memory_space=pl.ANY)
        return pl.pallas_call(
            functools.partial(kernel, side, n_expert // experts),
            out_shape=jax.ShapeDtypeStruct((rows, 2 * width), BF16),
            in_specs=[hbm] * 6,
            out_specs=pl.BlockSpec(memory_space=pltpu.VMEM),
            scratch_shapes=scratch,
            compiler_params=pltpu.CompilerParams(
                collective_id=0, has_side_effects=True, vmem_limit_bytes=60 * 1024 * 1024
            ),
            name="moe_layer",
        )(tokens, routes.T, router_logits.T, gate_weight, up_weight, down_weight)

    return jax.shard_map(
        layer,
        mesh=mesh,
        in_specs=(
            P(("groups", "expert"), None),
            P(("groups", "expert"), None),
            P(("groups", "expert"), None),
            P("expert", None, "tensor"),
            P("expert", None, "tensor"),
            P("expert", "tensor", None),
        ),
        out_specs=P(("groups", "expert"), "tensor"),
        check_vma=False,
    )
```

```python
import functools
import math

import jax
import jax.numpy as jnp
from jax import lax
from jax.experimental import pallas as pl
from jax.experimental.pallas import tpu as pltpu
from jax.sharding import PartitionSpec as P

MESH = pl.DeviceIdType.MESH
F32, BF16 = jnp.float32, jnp.bfloat16
LANES = 128


def ring_order(side):
    order = [0]
    for k in range(1, side // 2):
        order += [k, side - k]
    return order + [side // 2]


def kernel(
    side, segs, tok, routes, logits, gate, up, down, out,
    named, scores, gu, wd, own, sib, pre, hid, hmir, wall, wcol, part, csend, crecv, fsend, frecv,
    load_sem, p1_send, p1_recv, ring_send, ring_recv, d2d_send, d2d_recv,
    w1_send, w1_recv, w2_send, w2_recv, x_send, x_recv,
    cr_send, cr_recv, f_send, f_recv,
):
    order = ring_order(side)
    pos = {k: p for p, k in enumerate(order)}
    mirror = [pos[(side - k) % side] for k in order]
    cuts = [0, 1] + list(range(3, side - 2, 2)) + [side]
    blocks = list(zip(cuts[:-1], cuts[1:]))
    nb = len(blocks)
    rows, width = own.shape[3], own.shape[4]
    hc = wd.shape[0] // 2
    hops = (side // 2, side // 2 - 1)
    x_pieces = x_send.shape[0] - side

    core = lax.axis_index("tensor")
    place = lax.axis_index("expert")
    y, x = place // side, lax.rem(place, side)
    expert = place // segs
    sign = 1 - 2 * core

    def along(axis, k):
        step = sign * k + side
        if axis == 0:
            return {"expert": lax.rem(y + step, side) * side + x}
        return {"expert": y * side + lax.rem(x + step, side)}

    def remote(src, dst, send, recv, device):
        return pltpu.make_async_remote_copy(
            src_ref=src, dst_ref=dst, send_sem=send, recv_sem=recv, device_id=device, device_id_type=MESH
        )

    other = {"tensor": 1 - core}
    started = []

    def start(copy):
        copy.start()
        started.append(copy)

    def arrived(ref, send, recv):
        remote(ref, ref, send, recv, other).wait_recv()

    half = 2 * width
    tok_loads = [
        pltpu.make_async_copy(
            tok.at[:, pl.ds(pl.multiple_of(core * half + t * width, LANES), width)], own.at[t, 0, 0], load_sem.at[t]
        )
        for t in range(2)
    ]
    small_loads = [
        pltpu.make_async_copy(routes, named, load_sem.at[2]),
        pltpu.make_async_copy(logits, scores, load_sem.at[12]),
    ]
    for copy in tok_loads + small_loads:
        copy.start()
    loads = []
    for q in range(4):
        who = core if q < 2 else 1 - core
        first = pl.multiple_of(who * half + (q % 2) * width, LANES)
        for i, matrix in enumerate((gate, up)):
            loads.append(
                pltpu.make_async_copy(
                    matrix.at[0, pl.ds(first, width), :], gu.at[q, :, pl.ds(i * hc, hc)], load_sem.at[4 + 2 * q + i]
                )
            )
    wd_load = pltpu.make_async_copy(
        down.at[0, :, pl.ds(pl.multiple_of(core * half, LANES), half)], wd.at[:hc], load_sem.at[3]
    )
    wd_load.start()

    barrier = pltpu.get_barrier_semaphore()
    for k in range(1, side):
        for axis in range(2):
            pl.semaphore_signal(barrier, inc=1, device_id=along(axis, k), device_id_type=MESH)
    pl.semaphore_signal(barrier, inc=1, device_id=other, device_id_type=MESH)
    for copy in tok_loads:
        copy.wait()
    pl.semaphore_wait(barrier, 2 * (side - 1) + 1)

    def pass_on(t, k):
        back = pos[side - k]
        start(remote(own.at[t, 0, 0], own.at[t, 0, back], p1_send.at[t, back], p1_recv.at[t, back], along(t, k)))

    def forward(t, d, h, b):
        lo, hi = blocks[b]
        k = (side - h) % side if d == 0 else h
        k_there = (side - h - 1) % side if d == 0 else h + 1
        start(remote(
            own.at[t, pos[k], lo:hi], own.at[t, pos[k_there], lo:hi],
            ring_send.at[t, d, h, b], ring_recv.at[t, pos[k_there], b], along(1 - t, 1 if d == 0 else side - 1),
        ))

    def span_of(h):
        return (0, 1) if h == 0 else (2 * h - 1, min(2 * h + 1, side))

    def project(src, t, q, h, mirrored):
        first, last = span_of(h)
        r = jnp.dot(src[t, first:last].reshape((last - first) * side * rows, width), gu[q], preferred_element_type=F32)
        r = r.reshape(last - first, side, rows, 2 * hc)
        for c in range(first, last):
            for p in range(side):
                at = (mirror[c], mirror[p]) if mirrored else (c, p)
                i, j = at if t == 0 else at[::-1]
                pre[i, j] += r[c - first, p]

    def own_dots(h):
        for t in range(2):
            project(own, t, t, h, False)

    def sib_dots(h):
        for t in range(2):
            for chunk in range(*span_of(h)):
                for b, (lo, hi) in enumerate(blocks):
                    arrived(sib.at[t, chunk, lo:hi], d2d_send.at[t, chunk, b], d2d_recv.at[t, chunk, b])
            project(sib, t, 2 + t, h, True)

    for h, b in [(h, b) for h in range(side // 2 + 1) for b in range(nb)]:
        step = h * nb + b
        here = []
        lo, hi = blocks[b]
        for t in range(2):
            if step == 0:
                pass_on(t, order[1])
                pass_on(t, order[2])
            for d in range(2):
                if h > hops[d]:
                    continue
                chunk = pos[(side - h) % side if d == 0 else h]
                if h > 0:
                    arrived(own.at[t, chunk, lo:hi], ring_send.at[t, 0, 0, b], ring_recv.at[t, chunk, b])
                elif d == 0:
                    for p in range(max(lo, 1), hi):
                        arrived(own.at[t, 0, p], p1_send.at[t, p], p1_recv.at[t, p])
                if h < hops[d]:
                    forward(t, d, h, b)
                if h > 0 or d == 0:
                    here.append((t, chunk, b))
            if step == 0:
                for k in order[3:]:
                    pass_on(t, k)
        for t, chunk, b in here:
            lo, hi = blocks[b]
            start(remote(
                own.at[t, chunk, lo:hi], sib.at[t, chunk, lo:hi], d2d_send.at[t, chunk, b], d2d_recv.at[t, chunk, b], other
            ))
        if step < x_pieces:
            span = half // x_pieces
            start(remote(
                down.at[0, :, pl.ds(pl.multiple_of((1 - core) * half + step * span, LANES), span)],
                wd.at[hc:, step * span:(step + 1) * span], x_send.at[step], x_recv.at[step], other,
            ))
        if step == 0:
            for copy in loads:
                copy.start()
            pre[...] = jnp.zeros_like(pre)
            for copy in small_loads:
                copy.wait()
            experts = scores.shape[0]
            picked = [
                sum(jnp.where(named[k:k + 1, :] == e, scores[e:e + 1, :], 0.0) for e in range(experts)) for k in range(2)
            ]
            top = jnp.maximum(picked[0], picked[1])
            raised = [jnp.exp(v - top) for v in picked]
            weight = [v / (raised[0] + raised[1]) for v in raised]
            wall[0, 0] = jnp.zeros_like(wall[0, 0])
            for e in range(experts):
                wall[0, 0, :, e * rows:(e + 1) * rows] = sum(
                    jnp.where(named[k:k + 1, :] == e, weight[k], 0.0) for k in range(2)
                )
        if step == nb:
            for k in order[1:]:
                back = pos[side - k]
                start(remote(wall.at[0, 0], wall.at[0, back], w1_send.at[back], w1_recv.at[back], along(0, k)))
        if step == 2 * nb:
            for p in range(1, side):
                arrived(wall.at[0, p], w1_send.at[p], w1_recv.at[p])
            for k in order[1:]:
                back = pos[side - k]
                start(remote(wall.at[0], wall.at[back], w2_send.at[back], w2_recv.at[back], along(1, k)))
        if h == 1 and b == 1:
            for copy in loads:
                copy.wait()
        if h > 0 and b == 1:
            own_dots(h - 1)
        if h > 0 and b == min(2, nb - 1):
            sib_dots(h - 1)
    own_dots(side // 2)
    sib_dots(side // 2)

    for i in reversed(range(side)):
        g, u = pre[i, :, :, :hc], pre[i, :, :, hc:]
        h_here = (g / (1.0 + jnp.exp(-g)) * u).astype(BF16)
        hid[i, :, :, :hc] = h_here
        for j in range(side):
            hmir[mirror[i], mirror[j]] = h_here[j]
        m = mirror[i]
        start(remote(hmir.at[m], hid.at[m, :, :, hc:], x_send.at[x_pieces + m], x_recv.at[x_pieces + m], other))

    def other_hidden(first, last):
        for i in range(first, last):
            arrived(hid.at[i, :, :, hc:], x_send.at[x_pieces + i], x_recv.at[x_pieces + i])

    for p in range(1, side):
        arrived(wall.at[p], w2_send.at[p], w2_recv.at[p])
    lane = lax.broadcasted_iota(jnp.int32, (side, rows, LANES), 2)
    row = lax.broadcasted_iota(jnp.int32, (side, rows, LANES), 1)
    for i in range(side):
        spread = jnp.broadcast_to(wall[i], (side, rows, LANES))
        wcol[i] = jnp.sum(jnp.where(lane == expert * rows + row, spread, 0.0), axis=2, keepdims=True)

    wd_load.wait()
    for i in range(x_pieces):
        span = half // x_pieces
        arrived(wd.at[hc:, i * span:(i + 1) * span], x_send.at[i], x_recv.at[i])

    def make_parts(t, first):
        a = hid[first:first + 2] if t == 0 else hid[:, first:first + 2]
        r = jnp.dot(
            a.reshape(2 * side * rows, 2 * hc), wd[:, t * width:(t + 1) * width], preferred_element_type=F32
        )
        if t == 0:
            part[t, first:first + 2] = r.reshape(2, side, rows, width) * wcol[first:first + 2]
        else:
            r = r.reshape(side, 2, rows, width)
            for c in range(2):
                part[t, first + c] = r[:, c] * wcol[:, first + c]

    back_blocks = blocks[::-1]
    drained = 0
    for h in range(side // 2):
        before = len(started)
        first = side - 2 - 2 * h
        halves = [(t, b) for t in range(2) for b in range(nb)] if h == 0 else [(t, b) for b in range(nb) for t in range(2)]
        for t, b in halves:
            if h == 0 and b == 0:
                other_hidden(*((first, side) if t == 0 else (0, first)))
                make_parts(t, first)
            lo, hi = back_blocks[b]
            for d in range(2):
                if h >= hops[d]:
                    continue
                k = hops[d] - h if d == 0 else side - hops[d] + h
                value = part[t, pos[k], lo:hi]
                if h > 0:
                    arrived(crecv.at[t, d, h, lo:hi], cr_send.at[t, 0, 0, b], cr_recv.at[t, d, h, b])
                    value = value + crecv[t, d, h, lo:hi].astype(F32)
                csend[t, d, h, lo:hi] = value.astype(BF16)
                start(remote(
                    csend.at[t, d, h, lo:hi], crecv.at[t, d, h + 1, lo:hi],
                    cr_send.at[t, d, h, b], cr_recv.at[t, d, h + 1, b], along(1 - t, 1 if d == 0 else side - 1),
                ))
        if h + 1 < side // 2:
            for t in range(2):
                make_parts(t, first - 2)
        for copy in started[drained:before]:
            copy.wait_send()
        drained = before
    for b in range(nb):
        lo, hi = back_blocks[b]
        for t in range(2):
            total = part[t, 0, lo:hi]
            for d in range(2):
                arrived(crecv.at[t, d, hops[d], lo:hi], cr_send.at[t, 0, 0, b], cr_recv.at[t, d, hops[d], b])
                total = total + crecv[t, d, hops[d], lo:hi].astype(F32)
            part[t, 0, lo:hi] = total
            fsend[t, lo:hi] = total.astype(BF16)
            for p in reversed(range(max(lo, 1), hi)):
                back = pos[side - order[p]]
                start(remote(
                    fsend.at[t, p], frecv.at[t, back], f_send.at[t, back], f_recv.at[t, back], along(t, order[p])
                ))
    for t in range(2):
        total = part[t, 0, 0]
        for p in range(1, side):
            arrived(frecv.at[t, p], f_send.at[t, p], f_recv.at[t, p])
            total = total + frecv[t, p].astype(F32)
        out[:, t * width:(t + 1) * width] = total.astype(out.dtype)
    for copy in started[drained:]:
        copy.wait_send()


def solution(mesh):
    n_expert = mesh.shape["expert"]
    side = math.isqrt(n_expert)
    nb = len([0, 1] + list(range(3, side - 2, 2)))

    def layer(tokens, routes, router_logits, gate_weight, up_weight, down_weight):
        rows, width = tokens.shape[0], tokens.shape[1] // 4
        experts = router_logits.shape[1]
        hc = down_weight.shape[1]
        hop = side // 2
        pieces = math.gcd(2 * width // LANES, side)
        dma = pltpu.SemaphoreType.DMA
        scratch = [
            pltpu.VMEM((routes.shape[1], rows), jnp.int32),
            pltpu.VMEM((experts, rows), F32),
            pltpu.VMEM((4, width, 2 * hc), BF16),
            pltpu.VMEM((2 * hc, 2 * width), BF16),
            pltpu.VMEM((2, side, side, rows, width), BF16),
            pltpu.VMEM((2, side, side, rows, width), BF16),
            pltpu.VMEM((side, side, rows, 2 * hc), F32),
            pltpu.VMEM((side, side, rows, 2 * hc), BF16),
            pltpu.VMEM((side, side, rows, hc), BF16),
            pltpu.VMEM((side, side, 1, LANES), F32),
            pltpu.VMEM((side, side, rows, 1), F32),
            pltpu.VMEM((2, side, side, rows, width), F32),
            pltpu.VMEM((2, 2, hop, side, rows, width), BF16),
            pltpu.VMEM((2, 2, hop + 1, side, rows, width), BF16),
            pltpu.VMEM((2, side, rows, width), BF16),
            pltpu.VMEM((2, side, rows, width), BF16),
            dma((13,)),
            dma((2, side)), dma((2, side)),
            dma((2, 2, hop, nb)), dma((2, side, nb)),
            dma((2, side, nb)), dma((2, side, nb)),
            dma((side,)), dma((side,)), dma((side,)), dma((side,)),
            dma((pieces + side,)), dma((pieces + side,)),
            dma((2, 2, hop, nb)), dma((2, 2, hop + 1, nb)),
            dma((2, side)), dma((2, side)),
        ]
        hbm = pl.BlockSpec(memory_space=pl.ANY)
        return pl.pallas_call(
            functools.partial(kernel, side, n_expert // experts),
            out_shape=jax.ShapeDtypeStruct((rows, 2 * width), BF16),
            in_specs=[hbm] * 6,
            out_specs=pl.BlockSpec(memory_space=pltpu.VMEM),
            scratch_shapes=scratch,
            compiler_params=pltpu.CompilerParams(
                collective_id=0, has_side_effects=True, vmem_limit_bytes=60 * 1024 * 1024
            ),
            name="moe_layer",
        )(tokens, routes.T, router_logits.T, gate_weight, up_weight, down_weight)

    return jax.shard_map(
        layer,
        mesh=mesh,
        in_specs=(
            P(("groups", "expert"), None),
            P(("groups", "expert"), None),
            P(("groups", "expert"), None),
            P("expert", None, "tensor"),
            P("expert", None, "tensor"),
            P("expert", "tensor", None),
        ),
        out_specs=P(("groups", "expert"), "tensor"),
        check_vma=False,
    )
```
